768 devices in a mesh: wave: 12 (over z), lev: 8 (over y), grp: 8 (over x, core).
Axes of the slice: x: 4, y: 8, z: 12, core: 2. Of those that a mesh axis runs over, the one named last changes fastest.
Arguments:
- spectra: bfloat16 [2, 4, 8, 96, 1024], P(None, None, 'lev', ('wave', 'grp')), may hold values from -6 to 6
- legendre: bfloat16 [96, 1024, 384], P(('wave', 'grp')), may hold values from -0.1875 to 0.1875
- wavenumbers: int32 [96], replicated, may hold values from 0 to 1023, as said below
- quad_weights: float32 [384], replicated, may hold values from 0.5 to 2
- tracers: float32 [8, 8, 384, 4096], P(None, 'lev', ('wave', 'grp')), may hold values from 0.2 to 2
- kinetics: float32 [8, 8], replicated, may hold values from -2 to 2
- photolysis: float32 [8], replicated, may hold values from -1 to 1
- heat_weights: float32 [3, 8], replicated, may hold values from -2 to 2
Outputs:
- tracers_out: float32 [8, 8, 384, 4096], P(None, 'lev', ('wave', 'grp'))
- heating_spectra: float32 [2, 3, 8, 96, 1024], P(None, None, 'lev', ('wave', 'grp'))
The draws below stay inside these ranges and needn't reach their ends.
Inputs may be any that keep to these rules, and one draw needn't show every extreme that they name: `wavenumbers`: ascending and distinct; slot s holds a value from s * (10) to (s + 1) * 10 - 1.
All inputs are finite; a program needn't handle non-finite values.
Results may differ from the reference program's by a relative error of at most 0.0025.
Values sent between devices are 32-bit elements; how exact they have to be, the bound alone decides.
A program may use at most 32 MiB of HBM per device.

```python
import math
import jax
import jax.numpy as jnp
from jax import lax

NDEG = 1024
NLON = 4096
FIELDS = 4
TRACERS = 8
HEATS = 3
LEVELS = 8
MW = 96
LATW = 384


def draw_wavenumbers(key, part):
    spacing = NDEG // MW
    offsets = jax.random.randint(jax.random.fold_in(key, 7), (MW,), 0, spacing, dtype=jnp.int32)
    return (jnp.arange(MW, dtype=jnp.int32) * spacing + offsets).astype(jnp.int32)


def block_levels(rng, shape, pieces, least, top_value):
    level, own = 1.0, jax.random.fold_in(rng, 6)
    for position, parts in pieces:
        heights = jnp.exp(jax.random.uniform(jax.random.fold_in(own, position), (parts,), jnp.float32, least / len(pieces), top_value / len(pieces)))
        level = level * jnp.repeat(heights, shape[position] // parts).reshape([-1 if axis == position else 1 for axis in range(len(shape))])
    return level


def gaussian(own_key, extent, width, most, pieces=(), held_as=jnp.bfloat16):
    drawn = width * jax.random.normal(own_key, extent, jnp.float32)
    if pieces:
        drawn = drawn * block_levels(own_key, extent, pieces, -0.22, 0.18)
    return jnp.clip(drawn, -most, most).astype(held_as)


def setup_inputs(seed: int = 0) -> dict:
    arg_keys = jax.random.split(jax.random.key(seed), 9)
    return {
        "spectra": gaussian(arg_keys[0], (2, FIELDS, LEVELS, MW, NDEG), 1.0, 6.0, ((2, 8), (3, 96))),
        "legendre": gaussian(arg_keys[1], (MW, NDEG, LATW), NDEG ** -0.5, 0.1875, ((0, 96),)),
        "wavenumbers": draw_wavenumbers(jax.random.fold_in(arg_keys[8], 71), 0),
        "quad_weights": jnp.clip(jnp.exp(jax.random.uniform(arg_keys[3], (LATW,), jnp.float32, math.log(0.5), math.log(2.0))), 0.5, 2.0),
        "tracers": jnp.clip(jnp.exp(math.log(2.0) - 2.3025851 * jax.random.uniform(arg_keys[4], (TRACERS, LEVELS, LATW, NLON), jnp.float32) ** block_levels(arg_keys[4], (TRACERS, LEVELS, LATW, NLON), ((1, 8), (2, 96)), -0.2, 0.2)), 0.2, 2.0),
        "kinetics": gaussian(arg_keys[5], (TRACERS, TRACERS), TRACERS ** -0.5, 2.0, (), jnp.float32),
        "photolysis": jnp.clip(jax.random.uniform(arg_keys[6], (TRACERS,), jnp.float32, -1.0, 1.0), -1.0, 1.0),
        "heat_weights": gaussian(arg_keys[7], (HEATS, TRACERS), TRACERS ** -0.5, 2.0, (), jnp.float32),
    }


highest = lax.Precision.HIGHEST

def fourier_table(wavenumbers):
    longitudes = jnp.arange(NLON, dtype=jnp.int32)
    phase_index = wavenumbers[:, None] * longitudes[None, :] % NLON
    angles = phase_index.astype(jnp.float32) * (2.0 * math.pi / NLON)
    return jnp.stack([jnp.cos(angles), -jnp.sin(angles)])

def advect(padded, courant_x, courant_y):
    centre = padded[..., 1:-1, :]
    northern = padded[..., :-2, :]
    southern = padded[..., 2:, :]
    western = jnp.roll(centre, 1, axis=-1)
    eastern = jnp.roll(centre, -1, axis=-1)
    return centre - jnp.maximum(courant_x, 0.0) * (centre - western) - jnp.minimum(courant_x, 0.0) * (eastern - centre) - jnp.maximum(courant_y, 0.0) * (centre - northern) - jnp.minimum(courant_y, 0.0) * (southern - centre)

def react(tracer_now, react_rate, photo_rate, kinetics, photolysis):
    mixed = jnp.tensordot(kinetics, tracer_now, axes=1, precision=highest)
    yields = photolysis.reshape((-1,) + (1,) * (tracer_now.ndim - 1))
    return tracer_now + 0.2 * react_rate * mixed + 0.2 * photo_rate * yields * tracer_now[0]

def reference(spectra, legendre, wavenumbers, quad_weights, tracers, kinetics, photolysis, heat_weights):
    degree_mask = jnp.arange(NDEG, dtype=jnp.int32)[None, :] < (NDEG - wavenumbers)[:, None]
    masked_coeffs = jnp.where(degree_mask, spectra.astype(jnp.float32), jnp.zeros((), jnp.float32))
    legendre_wide = legendre.astype(jnp.float32)
    fourier = jnp.einsum('pflsj,sjy->pflsy', masked_coeffs, legendre_wide, precision=highest)
    shared_table = fourier_table(wavenumbers)
    grid_fields = jnp.einsum('pflsy,psx->flyx', fourier, shared_table, precision=highest) * (1.0 / math.sqrt(MW))
    courant_x = 0.45 * jnp.tanh(grid_fields[0])
    courant_y = 0.45 * jnp.tanh(grid_fields[1])
    react_rate = jnp.exp(0.3 * grid_fields[2])
    running_sum = jnp.cumsum(tracers[0], axis=0)
    overhead = jnp.concatenate([jnp.zeros_like(running_sum[:1]), running_sum[:-1]], axis=0)
    photo_rate = jnp.exp(-2.0 * overhead / LEVELS)
    tracer_now = tracers
    for substep in range(2):
        padded = jnp.pad(tracer_now, ((0, 0), (0, 0), (1, 1), (0, 0)))
        tracer_now = react(advect(padded, courant_x, courant_y), react_rate, photo_rate, kinetics, photolysis)
    heating = jnp.tensordot(heat_weights, tracer_now, axes=1, precision=highest) * (1.0 + 0.5 * jnp.tanh(grid_fields[3]))
    heat_fourier = jnp.einsum('klyx,psx->pklsy', heating, shared_table, precision=highest) * (1.0 / math.sqrt(NLON))
    weighted = (heat_fourier * quad_weights).astype(jnp.bfloat16)
    heating_spectra = jnp.einsum('pklsy,sjy->pklsj', weighted.astype(jnp.float32), legendre_wide, precision=highest)
    heating_spectra = jnp.where(degree_mask, heating_spectra, jnp.zeros((), jnp.float32))
    return (tracer_now, heating_spectra)
```

```python
import math

import jax
import jax.numpy as jnp
from jax import lax
from jax.experimental import pallas as pl
from jax.experimental.pallas import tpu as pltpu
from jax.sharding import PartitionSpec as P

NW, NL, NG = 12, 8, 8
NPOS = NW * NG
NDEG = 1024
NLON = 4096
NLAT = 384
CHUNK = NLON // NL
F32 = jnp.float32
BF16 = jnp.bfloat16
MESH = pl.DeviceIdType.MESH
NT = (((1,), (1,)), ((), ()))
FAR_W = (6, 5, 7, 4, 8, 3, 9, 2, 10, 1, 11)
FAR_G = (4, 3, 5, 2, 6, 7, 1)
FAR_L = (4, 3, 5, 2, 6, 1, 7)


def cos_sin(m):
    shifted = m + NLON // 8
    quarter = (shifted >> 10) & 3
    angle = ((shifted & (NLON // 4 - 1)) - NLON // 8).astype(F32) * (2.0 * math.pi / NLON)
    z = angle * angle
    s = angle * (1.0 + z * (-1.0 / 6 + z * (1.0 / 120 + z * (-1.0 / 5040 + z * (1.0 / 362880)))))
    c = 1.0 + z * (-0.5 + z * (1.0 / 24 + z * (-1.0 / 720 + z * (1.0 / 40320))))
    odd = (quarter & 1) == 1
    cos = jnp.where(odd, s, c)
    sin = jnp.where(odd, c, s)
    cos = jnp.where(((quarter + 1) & 2) == 2, -cos, cos)
    sin = jnp.where((quarter & 2) == 2, -sin, sin)
    return cos, sin


def split(x):
    hi = x.astype(BF16)
    return hi, (x - hi.astype(F32)).astype(BF16)


def dot3(x, bh, bl, dims):
    hi, lo = split(x)
    out = lax.dot_general(hi, bh, dims, preferred_element_type=F32)
    out += lax.dot_general(lo, bh, dims, preferred_element_type=F32)
    return out + lax.dot_general(hi, bl, dims, preferred_element_type=F32)


def kernel(
    spec, leg, wn, quad, trc, kin, pho, hw,
    tout, sout,
    C, D, O, LV, X, T, S, Z1, G1, V, LR, PC, PH, COEF, AT, BH, BL, H, HF, S2, Z2, G2, WT, WC,
    local, zs, zr, gs, gr, ls, lr, ps, pr, es, er, hs, hr, zs2, zr2, gs2, gr2,
):
    w = lax.axis_index("wave")
    l = lax.axis_index("lev")
    g = lax.axis_index("grp")
    pos = w * NG + g
    up = lax.rem(pos + 1, NPOS)
    down = lax.rem(pos + NPOS - 1, NPOS)
    up_w, up_g = up // NG, lax.rem(up, NG)
    down_w, down_g = down // NG, lax.rem(down, NG)

    for i in range(4):
        rows = pl.ds(256 * i, 256)
        pltpu.make_async_copy(leg.at[0, rows, :], LV.at[rows, :], local.at[i]).start()
    own_rows = pltpu.make_async_copy(trc.at[:, 0], C.at[:, pl.ds(2, 4), :], local.at[4])
    own_rows.start()
    PH[...] = jnp.zeros_like(PH)

    barrier = pltpu.get_barrier_semaphore()

    def hello(dw, dl, dg):
        pl.semaphore_signal(barrier, inc=1, device_id=(dw, dl, dg), device_id_type=MESH)

    for k in FAR_W:
        hello(lax.rem(w + k, NW), l, g)
    for k in range(NL):
        ll = lax.rem(l + k, NL)
        hello(up_w, ll, up_g)
        hello(down_w, ll, down_g)
        if k:
            hello(w, ll, g)
    for k in FAR_G:
        hello(w, l, lax.rem(g + k, NG))
    count = (NW - 1) + (NG - 1) + (NL - 1) + 2 * NL

    own_wave = wn[pos]
    for p in range(2):
        for f in range(4):
            X[pl.ds(4 * p + f, 1), :] = spec[p, f, 0].astype(F32)
    degree = lax.broadcasted_iota(jnp.int32, (8, NDEG), 1)
    coeffs = jnp.where(degree < NDEG - own_wave, X[...], 0.0).astype(BF16)
    fourier = jnp.zeros((8, NLAT), F32)
    for i in range(4):
        rows = pl.ds(256 * i, 256)
        pltpu.make_async_copy(leg.at[0, rows, :], LV.at[rows, :], local.at[i]).wait()
        fourier += jnp.dot(
            coeffs[:, 256 * i : 256 * i + 256], LV[rows, :], preferred_element_type=F32
        )
    groups = []
    for c in range(2):
        for r in range(8):
            shift = (NLAT - (4 * c + r - 2)) % NLAT
            groups.append(pltpu.roll(fourier, shift, 1) if shift else fourier)
    T[...] = jnp.concatenate(groups, axis=0).T
    S[...] = T[pl.ds(0, 48, stride=8), :].reshape(NW, 4, 128)
    own_rows.wait()

    pl.semaphore_wait(barrier, count)

    def z_copy(src, dst, ssem, rsem, k):
        there = lax.rem(w + k, NW)
        return pltpu.make_async_remote_copy(
            src.at[there], dst.at[w], ssem.at[k], rsem.at[w],
            device_id=(there, l, g), device_id_type=MESH,
        )

    def z_arrival(src, dst, ssem, rsem, k):
        there = lax.rem(w + k, NW)
        return pltpu.make_async_remote_copy(
            src.at[there], dst.at[there], ssem.at[k], rsem.at[there],
            device_id=(there, l, g), device_id_type=MESH,
        )

    def g_copy(src, dst, ssem, rsem, k, share):
        there = lax.rem(g + k, NG)
        return pltpu.make_async_remote_copy(
            src.at[:, there // share, :], dst.at[:, g, :], ssem.at[k], rsem.at[g],
            device_id=(w, l, there), device_id_type=MESH,
        )

    def g_arrival(src, dst, ssem, rsem, k, share):
        there = lax.rem(g + k, NG)
        return pltpu.make_async_remote_copy(
            src.at[:, there // share, :], dst.at[:, there, :], ssem.at[k], rsem.at[there],
            device_id=(w, l, there), device_id_type=MESH,
        )

    def l_copy(k, arrival=False):
        there = lax.rem(l + k, NL)
        return pltpu.make_async_remote_copy(
            C.at[0, pl.ds(2, 4), pl.ds(pl.multiple_of(CHUNK * there, CHUNK), CHUNK)],
            LR.at[there if arrival else l], ls.at[k], lr.at[there if arrival else l],
            device_id=(w, there, g), device_id_type=MESH,
        )

    def p_copy(k, arrival=False):
        there = lax.rem(l + k, NL)
        part = there if arrival else l
        return pltpu.make_async_remote_copy(
            PC.at[there],
            PH.at[pl.ds(2, 4), pl.ds(pl.multiple_of(CHUNK * part, CHUNK), CHUNK)],
            ps.at[k], pr.at[part],
            device_id=(w, there, g), device_id_type=MESH,
        )

    def e_copy(side, k, arrival=False):
        there = lax.rem(l + k, NL)
        part = there if arrival else l
        return pltpu.make_async_remote_copy(
            PC.at[there, pl.ds(3 if side else 0, 1)],
            PH.at[pl.ds(1 if side else 6, 1), pl.ds(pl.multiple_of(CHUNK * part, CHUNK), CHUNK)],
            es.at[side, k], er.at[side, part],
            device_id=(up_w, there, up_g) if side else (down_w, there, down_g),
            device_id_type=MESH,
        )

    def h_copy(side):
        return pltpu.make_async_remote_copy(
            C.at[:, pl.ds(4 if side else 2, 2), :],
            C.at[:, pl.ds(0 if side else 6, 2), :],
            hs.at[side], hr.at[side],
            device_id=(up_w, l, up_g) if side else (down_w, l, down_g),
            device_id_type=MESH,
        )

    for k in FAR_W:
        z_copy(S, Z1, zs, zr, k).start()
    for k in FAR_L:
        l_copy(k).start()
    for side in range(2):
        h_copy(side).start()
    Z1[w] = S[w]
    LR[l] = C[0, pl.ds(2, 4), pl.ds(pl.multiple_of(CHUNK * l, CHUNK), CHUNK)]

    for s in range(NPOS):
        WC[pl.ds(s, 1), :] = jnp.full((1, 128), wn[s], jnp.int32)
    WC[pl.ds(NPOS, 128 - NPOS), :] = jnp.zeros((128 - NPOS, 128), jnp.int32)
    waves = WC[...]
    across = waves.astype(F32).T[:16, :].astype(jnp.int32)
    coarse = lax.broadcasted_iota(jnp.int32, (16, 128), 0) * 256
    AT[0], AT[1] = cos_sin((across * coarse) & (NLON - 1))
    used = lax.broadcasted_iota(jnp.int32, (128, 128), 0) < NPOS
    for half in range(2):
        fine = lax.broadcasted_iota(jnp.int32, (128, 128), 1) + 128 * half
        cos, sin = cos_sin((waves * fine) & (NLON - 1))
        for p, table in enumerate((cos, -sin)):
            hi, lo = split(jnp.where(used, table, 0.0))
            BH[pl.ds(128 * p, 128), pl.ds(128 * half, 128)] = hi
            BL[pl.ds(128 * p, 128), pl.ds(128 * half, 128)] = lo

    for k in range(1, NL):
        l_copy(k, True).wait_recv()
    total = jnp.zeros((4, CHUNK), F32)
    for level in range(NL):
        PC[level] = 0.2 * jnp.exp(total * (-2.0 / NL))
        if level < NL - 1:
            total += LR[level]
    for k in FAR_L:
        p_copy(k).start()
    for k in range(NL):
        for side in range(2):
            e_copy(side, k).start()
    PH[pl.ds(2, 4), pl.ds(pl.multiple_of(CHUNK * l, CHUNK), CHUNK)] = PC[l]

    for k in range(1, NW):
        z_arrival(S, Z1, zs, zr, k).wait_recv()
    for k in FAR_G:
        g_copy(Z1, G1, gs, gr, k, 2).start()
    G1[:, pl.ds(g, 1), :] = Z1[:, pl.ds(g // 2, 1), :]

    for side in range(2):
        h_copy(side).wait_recv()

    @pl.when(pos == 0)
    def _():
        C[:, pl.ds(0, 2), :] = jnp.zeros((8, 2, NLON), F32)

    @pl.when(pos == NPOS - 1)
    def _():
        C[:, pl.ds(6, 2), :] = jnp.zeros((8, 2, NLON), F32)

    for k in range(1, NG):
        g_arrival(Z1, G1, gs, gr, k, 2).wait_recv()

    arrived = jnp.concatenate([G1[...].reshape(NPOS, 128), jnp.zeros((128 - NPOS, 128), F32)], axis=0)
    V[...] = arrived.T
    second = lax.rem(g, 2) == 1
    parts = []
    for p in range(2):
        fields = []
        for f in range(4):
            first = V[pl.ds(4 * p + f, 8, stride=8), :]
            other = V[pl.ds(64 + 4 * p + f, 8, stride=8), :]
            fields.append(jnp.where(second, other, first))
        parts.append(jnp.concatenate(fields, axis=0) * (1.0 / math.sqrt(NPOS)))
    real, imag = parts
    latitude = lax.broadcasted_iota(jnp.int32, (8, 256), 0) + (4 * pos - 2)
    inside = jnp.where((latitude >= 0) & (latitude < NLAT), 1.0, 0.0)
    bh, bl = BH[...], BL[...]
    for part in range(4):
        turned = []
        for i in range(4):
            h = 4 * part + i
            ca, sa = AT[0, pl.ds(h, 1), :], AT[1, pl.ds(h, 1), :]
            turned.append(
                jnp.concatenate([real * ca - imag * sa, real * sa + imag * ca], axis=1)
            )
        grid = dot3(jnp.concatenate(turned, axis=0), bh, bl, (((1,), (0,)), ((), ())))
        for i in range(4):
            cols = pl.ds(256 * (4 * part + i), 256)
            field = [grid[32 * i + 8 * f : 32 * i + 8 * f + 8, :] for f in range(4)]
            cx = 0.45 * jnp.tanh(field[0]) * inside
            cy = 0.45 * jnp.tanh(field[1]) * inside
            COEF[0, :, cols] = inside - jnp.abs(cx) - jnp.abs(cy)
            COEF[1, :, cols] = jnp.maximum(cx, 0.0)
            COEF[2, :, cols] = jnp.maximum(-cx, 0.0)
            COEF[3, :, cols] = jnp.maximum(cy, 0.0)
            COEF[4, :, cols] = jnp.maximum(-cy, 0.0)
            COEF[5, :, cols] = 0.2 * jnp.exp(0.3 * field[2])
            COEF[6, :, cols] = 1.0 + 0.5 * jnp.tanh(field[3])

    for k in range(NL):
        if k:
            p_copy(k, True).wait_recv()
        for side in range(2):
            e_copy(side, k, True).wait_recv()

    lane = lax.broadcasted_iota(jnp.int32, (8, 128), 1)

    def substep(src, dst, last):
        def block(b, carry):
            here = pl.ds(pl.multiple_of(b * 128, 128), 128)
            west = pl.ds(pl.multiple_of(lax.rem(b + 31, 32) * 128, 128), 128)
            east = pl.ds(pl.multiple_of(lax.rem(b + 1, 32) * 128, 128), 128)
            cc, xp, xm, yp, ym = [COEF[i, :, here] for i in range(5)]
            moved = []
            for t in range(8):
                c = src[t, :, here]
                western = pltpu.roll(jnp.where(lane == 127, src[t, :, west], c), 1, 1)
                eastern = pltpu.roll(jnp.where(lane == 0, src[t, :, east], c), 127, 1)
                northern = pltpu.roll(c, 1, 0)
                southern = pltpu.roll(c, 7, 0)
                moved.append(cc * c + xp * western + xm * eastern + yp * northern + ym * southern)
            rate = COEF[5, :, here]
            light = PH[:, here] * moved[0]
            done = []
            for i in range(8):
                mixed = kin[i, 0] * moved[0]
                for t in range(1, 8):
                    mixed += kin[i, t] * moved[t]
                done.append(moved[i] + rate * mixed + pho[i] * light)
                dst[i, :, here] = done[i]
            if last:
                gain = COEF[6, :, here]
                for k in range(3):
                    heat = hw[k, 0] * done[0]
                    for t in range(1, 8):
                        heat += hw[k, t] * done[t]
                    H[b, pl.ds(8 * k, 8), :] = heat * gain
            return carry

        lax.fori_loop(0, 32, block, 0, unroll=2)

    substep(C, D, False)
    substep(D, O, True)
    result = pltpu.make_async_copy(O.at[:, pl.ds(2, 4), :], tout.at[:, 0], local.at[5])
    result.start()

    zr_sum = jnp.zeros((24, 128), F32)
    zi_sum = jnp.zeros((24, 128), F32)
    for part in range(4):
        rows = []
        for i in range(4):
            h = 4 * part + i
            rows.append(jnp.concatenate([H[2 * h], H[2 * h + 1]], axis=1))
        spectrum = dot3(jnp.concatenate(rows, axis=0), bh, bl, NT)
        for i in range(4):
            h = 4 * part + i
            ca, sa = AT[0, pl.ds(h, 1), :], AT[1, pl.ds(h, 1), :]
            yc = spectrum[24 * i : 24 * i + 24, :128]
            ys = spectrum[24 * i : 24 * i + 24, 128:]
            zr_sum += ca * yc + sa * ys
            zi_sum += ca * ys - sa * yc
    scale = 1.0 / math.sqrt(NLON)
    HF[pl.ds(0, 24), :] = zr_sum * scale
    HF[pl.ds(24, 24), :] = zi_sum * scale
    HF[pl.ds(48, 16), :] = jnp.zeros((16, 128), F32)
    mine = jnp.concatenate([HF[pl.ds(r, 8, stride=8), :] for r in range(2, 6)], axis=0)
    V[...] = jnp.concatenate(
        [pltpu.roll(mine, 128 - d, 1) if d else mine for d in range(4)], axis=0
    ).T
    S2[...] = V[pl.ds(0, 24, stride=4), :].reshape(NW, 2, 128)
    for k in FAR_W:
        z_copy(S2, Z2, zs2, zr2, k).start()
    Z2[w] = S2[w]
    for k in range(1, NW):
        z_arrival(S2, Z2, zs2, zr2, k).wait_recv()
    for k in FAR_G:
        g_copy(Z2, G2, gs2, gr2, k, 4).start()
    G2[:, pl.ds(g, 1), :] = Z2[:, pl.ds(g // 4, 1), :]
    for k in range(1, NG):
        g_arrival(Z2, G2, gs2, gr2, k, 4).wait_recv()

    bands = G2[...].reshape(NPOS, 128)
    quarter = lax.rem(g, 4)
    bands = jnp.where(quarter == 1, pltpu.roll(bands, 96, 1), bands)
    bands = jnp.where(quarter == 2, pltpu.roll(bands, 64, 1), bands)
    bands = jnp.where(quarter == 3, pltpu.roll(bands, 32, 1), bands)
    for r in range(4):
        WT[pl.ds(r, NPOS, stride=4), :] = pltpu.roll(bands, 128 - 8 * r, 1) if r else bands
    weighted = (WT[...].T[:8, :] * quad[...]).astype(BF16)
    found = lax.dot_general(weighted, LV[...], NT, preferred_element_type=F32)
    found = jnp.where(degree < NDEG - own_wave, found, 0.0)
    for p in range(2):
        for k in range(3):
            sout[p, k, 0] = found[3 * p + k : 3 * p + k + 1, :]

    result.wait()
    for k in range(1, NW):
        z_copy(S, Z1, zs, zr, k).wait_send()
        z_copy(S2, Z2, zs2, zr2, k).wait_send()
    for k in range(1, NG):
        g_copy(Z1, G1, gs, gr, k, 2).wait_send()
        g_copy(Z2, G2, gs2, gr2, k, 4).wait_send()
    for k in range(NL):
        if k:
            l_copy(k).wait_send()
            p_copy(k).wait_send()
        for side in range(2):
            e_copy(side, k).wait_send()
    for side in range(2):
        h_copy(side).wait_send()


def body(spectra, legendre, wavenumbers, quad_weights, tracers, kinetics, photolysis, heat_weights):
    vmem = pl.BlockSpec(memory_space=pltpu.VMEM)
    smem = pl.BlockSpec(memory_space=pltpu.SMEM)
    hbm = pl.BlockSpec(memory_space=pl.ANY)
    V, DMA = pltpu.VMEM, pltpu.SemaphoreType.DMA
    return pl.pallas_call(
        kernel,
        out_shape=(
            jax.ShapeDtypeStruct((8, 1, 4, NLON), F32),
            jax.ShapeDtypeStruct((2, 3, 1, 1, NDEG), F32),
        ),
        in_specs=[vmem, hbm, smem, vmem, hbm, smem, smem, smem],
        out_specs=(hbm, vmem),
        scratch_shapes=[
            V((8, 8, NLON), F32), V((8, 8, NLON), F32), V((8, 8, NLON), F32),
            V((NDEG, NLAT), BF16), V((8, NDEG), F32),
            V((NLAT, 128), F32), V((NW, 4, 128), F32), V((NW, 4, 128), F32), V((NW, NG, 128), F32),
            V((128, 128), F32),
            V((NL, 4, CHUNK), F32), V((NL, 4, CHUNK), F32), V((8, NLON), F32),
            V((7, 8, NLON), F32),
            V((2, 16, 128), F32), V((256, 256), BF16), V((256, 256), BF16),
            V((32, 24, 128), F32), V((64, 128), F32),
            V((NW, 2, 128), F32), V((NW, 2, 128), F32), V((NW, NG, 128), F32),
            V((NLAT, 128), F32), V((128, 128), jnp.int32),
            DMA((6,)), DMA((NW,)), DMA((NW,)), DMA((NG,)), DMA((NG,)), DMA((NL,)), DMA((NL,)),
            DMA((NL,)), DMA((NL,)), DMA((2, NL)), DMA((2, NL)), DMA((2,)), DMA((2,)),
            DMA((NW,)), DMA((NW,)), DMA((NG,)), DMA((NG,)),
        ],
        compiler_params=pltpu.CompilerParams(collective_id=0, has_side_effects=True),
    )(
        spectra, legendre, wavenumbers, quad_weights.reshape(1, NLAT), tracers,
        kinetics, photolysis, heat_weights,
    )


def solution(mesh):
    return jax.shard_map(
        body,
        mesh=mesh,
        in_specs=(
            P(None, None, "lev", ("wave", "grp"), None),
            P(("wave", "grp"), None, None),
            P(),
            P(),
            P(None, "lev", ("wave", "grp"), None),
            P(),
            P(),
            P(),
        ),
        out_specs=(
            P(None, "lev", ("wave", "grp"), None),
            P(None, None, "lev", ("wave", "grp"), None),
        ),
        check_vma=False,
    )
```

```python
import math

import jax
import jax.numpy as jnp
from jax import lax
from jax.experimental import pallas as pl
from jax.experimental.pallas import tpu as pltpu
from jax.sharding import PartitionSpec as P

NW, NL, NG = 12, 8, 8
NPOS = NW * NG
NDEG = 1024
NLON = 4096
NLAT = 384
CHUNK = NLON // NL
F32 = jnp.float32
BF16 = jnp.bfloat16
MESH = pl.DeviceIdType.MESH
NT = (((1,), (1,)), ((), ()))
FAR_W = (6, 5, 7, 4, 8, 3, 9, 2, 10, 1, 11)
FAR_G = (4, 3, 5, 2, 6, 7, 1)
FAR_L = (4, 3, 5, 2, 6, 1, 7)


def cos_sin(m):
    shifted = m + NLON // 8
    quarter = (shifted >> 10) & 3
    angle = ((shifted & (NLON // 4 - 1)) - NLON // 8).astype(F32) * (2.0 * math.pi / NLON)
    z = angle * angle
    s = angle * (1.0 + z * (-1.0 / 6 + z * (1.0 / 120 + z * (-1.0 / 5040 + z * (1.0 / 362880)))))
    c = 1.0 + z * (-0.5 + z * (1.0 / 24 + z * (-1.0 / 720 + z * (1.0 / 40320))))
    odd = (quarter & 1) == 1
    cos = jnp.where(odd, s, c)
    sin = jnp.where(odd, c, s)
    cos = jnp.where(((quarter + 1) & 2) == 2, -cos, cos)
    sin = jnp.where((quarter & 2) == 2, -sin, sin)
    return cos, sin


def split(x):
    hi = x.astype(BF16)
    return hi, (x - hi.astype(F32)).astype(BF16)


def dot3(x, bh, bl, dims):
    hi, lo = split(x)
    out = lax.dot_general(hi, bh, dims, preferred_element_type=F32)
    out += lax.dot_general(lo, bh, dims, preferred_element_type=F32)
    return out + lax.dot_general(hi, bl, dims, preferred_element_type=F32)


def kernel(
    spec_in, leg, wn_in, quad_in, trc, kin_in, pho_in, hw_in,
    tout, sout,
    spec, wn, quad, kin, pho, hw, C, D, O, M, Q, HN, KP, LV, X, T, S, Z1, G1, V, LR, PC, PH, COEF, AT, BH, BL, H, HF, S2, Z2, G2, WT, WC,
    local, zs, zr, gs, gr, ls, lr, ps, pr, es, er, hs, hr, zs2, zr2, gs2, gr2,
):
    w = lax.axis_index("wave")
    l = lax.axis_index("lev")
    g = lax.axis_index("grp")
    pos = w * NG + g
    up = lax.rem(pos + 1, NPOS)
    down = lax.rem(pos + NPOS - 1, NPOS)
    up_w, up_g = up // NG, lax.rem(up, NG)
    down_w, down_g = down // NG, lax.rem(down, NG)

    barrier = pltpu.get_barrier_semaphore()

    def hello(dw, dl, dg):
        pl.semaphore_signal(barrier, inc=1, device_id=(dw, dl, dg), device_id_type=MESH)

    for k in FAR_W:
        hello(lax.rem(w + k, NW), l, g)
    for k in range(NL):
        ll = lax.rem(l + k, NL)
        hello(up_w, ll, up_g)
        hello(down_w, ll, down_g)
        if k:
            hello(w, ll, g)
    for k in FAR_G:
        hello(w, l, lax.rem(g + k, NG))
    count = (NW - 1) + (NG - 1) + (NL - 1) + 2 * NL

    for i in range(4):
        rows = pl.ds(256 * i, 256)
        pltpu.make_async_copy(leg.at[0, rows, :], LV.at[rows, :], local.at[i]).start()
    own_rows = pltpu.make_async_copy(trc.at[:, 0], C.at[:, pl.ds(2, 4), :], local.at[4])
    own_rows.start()
    small = [
        pltpu.make_async_copy(src, dst, local.at[6 + i])
        for i, (src, dst) in enumerate(
            ((spec_in, spec), (wn_in, wn), (quad_in, quad), (kin_in, kin), (pho_in, pho), (hw_in, hw))
        )
    ]
    for copy in small:
        copy.start()
    for row in (0, 7):
        PH[pl.ds(row, 1), :] = jnp.zeros((1, NLON), F32)

    small[0].wait()
    small[1].wait()
    own_wave = wn[pos]
    for p in range(2):
        for f in range(4):
            X[pl.ds(4 * p + f, 1), :] = spec[p, 0, 0, pl.ds(f, 1), :].astype(F32)
    degree = lax.broadcasted_iota(jnp.int32, (8, NDEG), 1)
    coeffs = jnp.where(degree < NDEG - own_wave, X[...], 0.0).astype(BF16)
    fourier = jnp.zeros((8, NLAT), F32)
    for i in range(4):
        rows = pl.ds(256 * i, 256)
        pltpu.make_async_copy(leg.at[0, rows, :], LV.at[rows, :], local.at[i]).wait()
        fourier += jnp.dot(
            coeffs[:, 256 * i : 256 * i + 256], LV[rows, :], preferred_element_type=F32
        )
    groups = []
    for c in range(2):
        for r in range(8):
            shift = (NLAT - (4 * c + r - 2)) % NLAT
            groups.append(pltpu.roll(fourier, shift, 1) if shift else fourier)
    T[...] = jnp.concatenate(groups, axis=0).T
    S[...] = T[pl.ds(0, 48, stride=8), :].reshape(NW, 4, 128)
    own_rows.wait()

    pl.semaphore_wait(barrier, count)

    def z_copy(src, dst, ssem, rsem, k):
        there = lax.rem(w + k, NW)
        return pltpu.make_async_remote_copy(
            src.at[there], dst.at[w], ssem.at[k], rsem.at[w],
            device_id=(there, l, g), device_id_type=MESH,
        )

    def z_arrival(src, dst, ssem, rsem, k):
        there = lax.rem(w + k, NW)
        return pltpu.make_async_remote_copy(
            src.at[there], dst.at[there], ssem.at[k], rsem.at[there],
            device_id=(there, l, g), device_id_type=MESH,
        )

    def g_copy(src, dst, ssem, rsem, k, share):
        there = lax.rem(g + k, NG)
        return pltpu.make_async_remote_copy(
            src.at[:, there // share, :], dst.at[:, g, :], ssem.at[k], rsem.at[g],
            device_id=(w, l, there), device_id_type=MESH,
        )

    def g_arrival(src, dst, ssem, rsem, k, share):
        there = lax.rem(g + k, NG)
        return pltpu.make_async_remote_copy(
            src.at[:, there // share, :], dst.at[:, there, :], ssem.at[k], rsem.at[there],
            device_id=(w, l, there), device_id_type=MESH,
        )

    def l_copy(k, arrival=False):
        there = lax.rem(l + k, NL)
        return pltpu.make_async_remote_copy(
            C.at[0, pl.ds(2, 4), pl.ds(pl.multiple_of(CHUNK * there, CHUNK), CHUNK)],
            LR.at[there if arrival else l], ls.at[k], lr.at[there if arrival else l],
            device_id=(w, there, g), device_id_type=MESH,
        )

    def p_copy(k, arrival=False):
        there = lax.rem(l + k, NL)
        part = there if arrival else l
        return pltpu.make_async_remote_copy(
            PC.at[there],
            PH.at[pl.ds(2, 4), pl.ds(pl.multiple_of(CHUNK * part, CHUNK), CHUNK)],
            ps.at[k], pr.at[part],
            device_id=(w, there, g), device_id_type=MESH,
        )

    def e_copy(side, k, arrival=False):
        there = lax.rem(l + k, NL)
        part = there if arrival else l
        return pltpu.make_async_remote_copy(
            PC.at[there, pl.ds(3 if side else 0, 1)],
            PH.at[pl.ds(1 if side else 6, 1), pl.ds(pl.multiple_of(CHUNK * part, CHUNK), CHUNK)],
            es.at[side, k], er.at[side, part],
            device_id=(up_w, there, up_g) if side else (down_w, there, down_g),
            device_id_type=MESH,
        )

    def h_copy(side):
        return pltpu.make_async_remote_copy(
            C.at[:, pl.ds(4 if side else 2, 2), :],
            C.at[:, pl.ds(0 if side else 6, 2), :],
            hs.at[side], hr.at[side],
            device_id=(up_w, l, up_g) if side else (down_w, l, down_g),
            device_id_type=MESH,
        )

    for k in FAR_W:
        z_copy(S, Z1, zs, zr, k).start()
    for k in FAR_L:
        l_copy(k).start()
    for side in range(2):
        h_copy(side).start()
    Z1[w] = S[w]
    LR[l] = C[0, pl.ds(2, 4), pl.ds(pl.multiple_of(CHUNK * l, CHUNK), CHUNK)]

    for s in range(NPOS):
        WC[pl.ds(s, 1), :] = jnp.full((1, 128), wn[s], jnp.int32)
    WC[pl.ds(NPOS, 128 - NPOS), :] = jnp.zeros((128 - NPOS, 128), jnp.int32)
    waves = WC[...]
    across = waves.astype(F32).T[:16, :].astype(jnp.int32)
    coarse = lax.broadcasted_iota(jnp.int32, (16, 128), 0) * 256
    AT[0], AT[1] = cos_sin((across * coarse) & (NLON - 1))
    used = lax.broadcasted_iota(jnp.int32, (128, 128), 0) < NPOS
    for half in range(2):
        fine = lax.broadcasted_iota(jnp.int32, (128, 128), 1) + 128 * half
        cos, sin = cos_sin((waves * fine) & (NLON - 1))
        for p, table in enumerate((cos, -sin)):
            hi, lo = split(jnp.where(used, table, 0.0))
            BH[pl.ds(128 * p, 128), pl.ds(128 * half, 128)] = hi
            BL[pl.ds(128 * p, 128), pl.ds(128 * half, 128)] = lo

    for k in range(1, NL):
        l_copy(k, True).wait_recv()
    total = jnp.zeros((4, CHUNK), F32)
    for level in range(NL):
        PC[level] = 0.2 * jnp.exp(total * (-2.0 / NL))
        if level < NL - 1:
            total += LR[level]
    for k in FAR_L:
        p_copy(k).start()
    for k in range(NL):
        for side in range(2):
            e_copy(side, k).start()
    PH[pl.ds(2, 4), pl.ds(pl.multiple_of(CHUNK * l, CHUNK), CHUNK)] = PC[l]

    for k in range(1, NW):
        z_arrival(S, Z1, zs, zr, k).wait_recv()
    for k in FAR_G:
        g_copy(Z1, G1, gs, gr, k, 2).start()
    G1[:, pl.ds(g, 1), :] = Z1[:, pl.ds(g // 2, 1), :]

    for side in range(2):
        h_copy(side).wait_recv()

    @pl.when(pos == 0)
    def _():
        C[:, pl.ds(0, 2), :] = jnp.zeros((8, 2, NLON), F32)

    @pl.when(pos == NPOS - 1)
    def _():
        C[:, pl.ds(6, 2), :] = jnp.zeros((8, 2, NLON), F32)

    for k in range(1, NG):
        g_arrival(Z1, G1, gs, gr, k, 2).wait_recv()

    arrived = jnp.concatenate([G1[...].reshape(NPOS, 128), jnp.zeros((128 - NPOS, 128), F32)], axis=0)
    V[...] = arrived.T
    second = lax.rem(g, 2) == 1
    parts = []
    for p in range(2):
        fields = []
        for f in range(4):
            first = V[pl.ds(4 * p + f, 8, stride=8), :]
            other = V[pl.ds(64 + 4 * p + f, 8, stride=8), :]
            fields.append(jnp.where(second, other, first))
        parts.append(jnp.concatenate(fields, axis=0) * (1.0 / math.sqrt(NPOS)))
    real, imag = parts
    latitude = lax.broadcasted_iota(jnp.int32, (8, 256), 0) + (4 * pos - 2)
    inside = jnp.where((latitude >= 0) & (latitude < NLAT), 1.0, 0.0)
    bh, bl = BH[...], BL[...]
    for part in range(4):
        turned = []
        for i in range(4):
            h = 4 * part + i
            ca, sa = AT[0, pl.ds(h, 1), :], AT[1, pl.ds(h, 1), :]
            turned.append(
                jnp.concatenate([real * ca - imag * sa, real * sa + imag * ca], axis=1)
            )
        grid = dot3(jnp.concatenate(turned, axis=0), bh, bl, (((1,), (0,)), ((), ())))
        for i in range(4):
            cols = pl.ds(256 * (4 * part + i), 256)
            field = [grid[32 * i + 8 * f : 32 * i + 8 * f + 8, :] for f in range(4)]
            cx = 0.45 * jnp.tanh(field[0]) * inside
            cy = 0.45 * jnp.tanh(field[1]) * inside
            COEF[0, :, cols] = inside - jnp.abs(cx) - jnp.abs(cy)
            COEF[1, :, cols] = jnp.maximum(cx, 0.0)
            COEF[2, :, cols] = jnp.maximum(-cx, 0.0)
            COEF[3, :, cols] = jnp.maximum(cy, 0.0)
            COEF[4, :, cols] = jnp.maximum(-cy, 0.0)
            COEF[5, :, cols] = 0.2 * jnp.exp(0.3 * field[2])
            COEF[6, :, cols] = 1.0 + 0.5 * jnp.tanh(field[3])

    for copy in small[2:]:
        copy.wait()
    lane = lax.broadcasted_iota(jnp.int32, (8, 128), 1)

    def transported(here, pick):
        b = here // 128
        west = pl.ds(pl.multiple_of(lax.rem(b + 31, 32) * 128, 128), 128)
        east = pl.ds(pl.multiple_of(lax.rem(b + 1, 32) * 128, 128), 128)
        here = pl.ds(pl.multiple_of(here, 128), 128)
        cc, xp, xm, yp, ym = [COEF[i, :, here] for i in range(5)]

        def of(t):
            c = pick(t, here)
            western = pltpu.roll(jnp.where(lane == 127, pick(t, west), c), 1, 1)
            eastern = pltpu.roll(jnp.where(lane == 0, pick(t, east), c), 127, 1)
            northern = pltpu.roll(c, 1, 0)
            southern = pltpu.roll(c, 7, 0)
            return cc * c + xp * western + xm * eastern + yp * northern + ym * southern

        return of

    def transport(src, dst):
        def block(b, carry):
            of = transported(b * 128, lambda t, cols: src[t, :, cols])
            for t in range(8):
                dst[t, :, pl.ds(pl.multiple_of(b * 128, 128), 128)] = of(t)
            return carry

        lax.fori_loop(0, 32, block, 0, unroll=2)

    def mix(src, dst, heats):
        def block(b, carry):
            cols = pl.ds(pl.multiple_of(b * 512, 512), 512)
            rate = COEF[5, :, cols]
            moved = [src[t, :, cols] for t in range(8)]
            heat = [None] * 3
            for i in range(8):
                mixed = kin[i, 0] * moved[0]
                for t in range(1, 8):
                    mixed += kin[i, t] * moved[t]
                done = moved[i] + rate * mixed
                dst[i, :, cols] = done
                if heats:
                    heat = [
                        hw[k, i] * done if old is None else old + hw[k, i] * done
                        for k, old in enumerate(heat)
                    ]
            if heats:
                for k in range(3):
                    HN[k, :, cols] = heat[k]
            return carry

        lax.fori_loop(0, 8, block, 0)

    transport(C, M)
    mix(M, D, False)
    transport(D, O)
    mix(O, D, True)
    for i in range(8):
        total = jnp.full((8, 128), kin[i, 0] * pho[0], F32)
        for t in range(1, 8):
            total += jnp.full((8, 128), kin[i, t] * pho[t], F32)
        KP[i] = total
    for k in range(3):
        first = jnp.full((8, 128), hw[k, 0] * pho[0], F32)
        second = hw[k, 0] * KP[0]
        for t in range(1, 8):
            first += jnp.full((8, 128), hw[k, t] * pho[t], F32)
            second += hw[k, t] * KP[t]
        KP[8 + k] = first
        KP[11 + k] = second

    for k in range(NL):
        if k:
            p_copy(k, True).wait_recv()
        for side in range(2):
            e_copy(side, k, True).wait_recv()
    Q[...] = PH[...] * M[0]

    def finish(b, carry):
        here = pl.ds(pl.multiple_of(b * 128, 128), 128)
        lit = transported(b * 128, lambda t, cols: Q[:, cols])(0)
        both = lit + PH[:, here] * (O[0, :, here] + pho[0] * lit)
        late = COEF[5, :, here] * lit
        for i in range(8):
            done = D[i, :, here] + (pho[i] * both + KP[i] * late)
            tout[i, 0, :, here] = done[2:6, :]
        gain = COEF[6, :, here]
        for k in range(3):
            H[b, pl.ds(8 * k, 8), :] = (HN[k, :, here] + (KP[8 + k] * both + KP[11 + k] * late)) * gain
        return carry

    lax.fori_loop(0, 32, finish, 0, unroll=2)

    zr_sum = jnp.zeros((24, 128), F32)
    zi_sum = jnp.zeros((24, 128), F32)
    for part in range(4):
        rows = []
        for i in range(4):
            h = 4 * part + i
            rows.append(jnp.concatenate([H[2 * h], H[2 * h + 1]], axis=1))
        spectrum = dot3(jnp.concatenate(rows, axis=0), bh, bl, NT)
        for i in range(4):
            h = 4 * part + i
            ca, sa = AT[0, pl.ds(h, 1), :], AT[1, pl.ds(h, 1), :]
            yc = spectrum[24 * i : 24 * i + 24, :128]
            ys = spectrum[24 * i : 24 * i + 24, 128:]
            zr_sum += ca * yc + sa * ys
            zi_sum += ca * ys - sa * yc
    scale = 1.0 / math.sqrt(NLON)
    HF[pl.ds(0, 24), :] = zr_sum * scale
    HF[pl.ds(24, 24), :] = zi_sum * scale
    HF[pl.ds(48, 16), :] = jnp.zeros((16, 128), F32)
    mine = jnp.concatenate([HF[pl.ds(r, 8, stride=8), :] for r in range(2, 6)], axis=0)
    V[...] = jnp.concatenate(
        [pltpu.roll(mine, 128 - d, 1) if d else mine for d in range(4)], axis=0
    ).T
    S2[...] = V[pl.ds(0, 24, stride=4), :].reshape(NW, 2, 128)
    for k in FAR_W:
        z_copy(S2, Z2, zs2, zr2, k).start()
    Z2[w] = S2[w]
    for k in range(1, NW):
        z_arrival(S2, Z2, zs2, zr2, k).wait_recv()
    for k in FAR_G:
        g_copy(Z2, G2, gs2, gr2, k, 4).start()
    G2[:, pl.ds(g, 1), :] = Z2[:, pl.ds(g // 4, 1), :]
    for k in range(1, NG):
        g_arrival(Z2, G2, gs2, gr2, k, 4).wait_recv()

    bands = G2[...].reshape(NPOS, 128)
    quarter = lax.rem(g, 4)
    bands = jnp.where(quarter == 1, pltpu.roll(bands, 96, 1), bands)
    bands = jnp.where(quarter == 2, pltpu.roll(bands, 64, 1), bands)
    bands = jnp.where(quarter == 3, pltpu.roll(bands, 32, 1), bands)
    for r in range(4):
        WT[pl.ds(r, NPOS, stride=4), :] = pltpu.roll(bands, 128 - 8 * r, 1) if r else bands
    weighted = (WT[...].T[:8, :] * quad[...].reshape(1, NLAT)).astype(BF16)
    found = lax.dot_general(weighted, LV[...], NT, preferred_element_type=F32)
    found = jnp.where(degree < NDEG - own_wave, found, 0.0)
    for p in range(2):
        for k in range(3):
            sout[p, k, 0] = found[3 * p + k : 3 * p + k + 1, :]

    for k in range(1, NW):
        z_copy(S, Z1, zs, zr, k).wait_send()
        z_copy(S2, Z2, zs2, zr2, k).wait_send()
    for k in range(1, NG):
        g_copy(Z1, G1, gs, gr, k, 2).wait_send()
        g_copy(Z2, G2, gs2, gr2, k, 4).wait_send()
    for k in range(NL):
        if k:
            l_copy(k).wait_send()
            p_copy(k).wait_send()
        for side in range(2):
            e_copy(side, k).wait_send()
    for side in range(2):
        h_copy(side).wait_send()


def body(spectra, legendre, wavenumbers, quad_weights, tracers, kinetics, photolysis, heat_weights):
    vmem = pl.BlockSpec(memory_space=pltpu.VMEM)
    hbm = pl.BlockSpec(memory_space=pl.ANY)
    V, DMA = pltpu.VMEM, pltpu.SemaphoreType.DMA
    return pl.pallas_call(
        kernel,
        out_shape=(
            V((8, 1, 4, NLON), F32),
            V((2, 3, 1, 1, NDEG), F32),
        ),
        in_specs=[hbm] * 8,
        out_specs=(vmem, vmem),
        scratch_shapes=[
            V((2, 1, 1, 4, NDEG), BF16), pltpu.SMEM((NPOS,), jnp.int32), V((NLAT,), F32),
            pltpu.SMEM((8, 8), F32), pltpu.SMEM((8,), F32), pltpu.SMEM((3, 8), F32),
            V((8, 8, NLON), F32), V((8, 8, NLON), F32), V((8, 8, NLON), F32), V((8, 8, NLON), F32),
            V((8, NLON), F32), V((3, 8, NLON), F32), V((14, 8, 128), F32),
            V((NDEG, NLAT), BF16), V((8, NDEG), F32),
            V((NLAT, 128), F32), V((NW, 4, 128), F32), V((NW, 4, 128), F32), V((NW, NG, 128), F32),
            V((128, 128), F32),
            V((NL, 4, CHUNK), F32), V((NL, 4, CHUNK), F32), V((8, NLON), F32),
            V((7, 8, NLON), F32),
            V((2, 16, 128), F32), V((256, 256), BF16), V((256, 256), BF16),
            V((32, 24, 128), F32), V((64, 128), F32),
            V((NW, 2, 128), F32), V((NW, 2, 128), F32), V((NW, NG, 128), F32),
            V((NLAT, 128), F32), V((128, 128), jnp.int32),
            DMA((12,)), DMA((NW,)), DMA((NW,)), DMA((NG,)), DMA((NG,)), DMA((NL,)), DMA((NL,)),
            DMA((NL,)), DMA((NL,)), DMA((2, NL)), DMA((2, NL)), DMA((2,)), DMA((2,)),
            DMA((NW,)), DMA((NW,)), DMA((NG,)), DMA((NG,)),
        ],
        compiler_params=pltpu.CompilerParams(collective_id=0, has_side_effects=True),
    )(
        spectra.transpose(0, 2, 3, 1, 4), legendre, wavenumbers, quad_weights, tracers, kinetics,
        photolysis, heat_weights,
    )


def solution(mesh):
    return jax.shard_map(
        body,
        mesh=mesh,
        in_specs=(
            P(None, None, "lev", ("wave", "grp"), None),
            P(("wave", "grp"), None, None),
            P(),
            P(),
            P(None, "lev", ("wave", "grp"), None),
            P(),
            P(),
            P(),
        ),
        out_specs=(
            P(None, "lev", ("wave", "grp"), None),
            P(None, None, "lev", ("wave", "grp"), None),
        ),
        check_vma=False,
    )
```

```python
import math

import jax
import jax.numpy as jnp
from jax import lax
from jax.experimental import pallas as pl
from jax.experimental.pallas import tpu as pltpu
from jax.sharding import PartitionSpec as P

NW, NL, NG = 12, 8, 8
NPOS = NW * NG
NDEG = 1024
NLON = 4096
NLAT = 384
CHUNK = NLON // NL
F32 = jnp.float32
BF16 = jnp.bfloat16
MESH = pl.DeviceIdType.MESH
NT = (((1,), (1,)), ((), ()))
FAR_W = (6, 5, 7, 4, 8, 3, 9, 2, 10, 1, 11)
FAR_G = (4, 3, 5, 2, 6, 7, 1)
FAR_L = (4, 3, 5, 2, 6, 1, 7)


def hops(peer):
    dw, dx = peer[0], peer[1] // 2
    return min(dw, NW - dw) + min(dx, NG // 2 - dx)


PEERS = sorted(((dw, dg) for dw in range(NW) for dg in range(NG) if dw or dg), key=hops, reverse=True)
LANES = pl.ds(0, 128)


def cos_sin(m):
    shifted = m + NLON // 8
    quarter = (shifted >> 10) & 3
    angle = ((shifted & (NLON // 4 - 1)) - NLON // 8).astype(F32) * (2.0 * math.pi / NLON)
    z = angle * angle
    s = angle * (1.0 + z * (-1.0 / 6 + z * (1.0 / 120 + z * (-1.0 / 5040 + z * (1.0 / 362880)))))
    c = 1.0 + z * (-0.5 + z * (1.0 / 24 + z * (-1.0 / 720 + z * (1.0 / 40320))))
    odd = (quarter & 1) == 1
    cos = jnp.where(odd, s, c)
    sin = jnp.where(odd, c, s)
    cos = jnp.where(((quarter + 1) & 2) == 2, -cos, cos)
    sin = jnp.where((quarter & 2) == 2, -sin, sin)
    return cos, sin


def split(x):
    hi = x.astype(BF16)
    return hi, (x - hi.astype(F32)).astype(BF16)


def dot3(x, bh, bl, dims):
    hi, lo = split(x)
    out = lax.dot_general(hi, bh, dims, preferred_element_type=F32)
    out += lax.dot_general(lo, bh, dims, preferred_element_type=F32)
    return out + lax.dot_general(hi, bl, dims, preferred_element_type=F32)


def kernel(
    spec_in, leg, wn_in, quad_in, trc, kin_in, pho_in, hw_in,
    tout, sout,
    spec, wn, quad, kin, pho, hw, C, D, O, M, Q, HN, KP, LV, X, T, S, Z1, G1, V, LR, PC, PH, COEF, AT, BH, BL, H, HF, S2, G2, WT, WC,
    local, zs, zr, gs, gr, ls, lr, ps, pr, es, er, hs, hr, zs2, zr2,
):
    w = lax.axis_index("wave")
    l = lax.axis_index("lev")
    g = lax.axis_index("grp")
    pos = w * NG + g
    up = lax.rem(pos + 1, NPOS)
    down = lax.rem(pos + NPOS - 1, NPOS)
    up_w, up_g = up // NG, lax.rem(up, NG)
    down_w, down_g = down // NG, lax.rem(down, NG)

    for i in range(4):
        rows = pl.ds(256 * i, 256)
        pltpu.make_async_copy(leg.at[0, rows, :], LV.at[rows, :], local.at[i]).start()
    own_rows = pltpu.make_async_copy(trc.at[:, 0], C.at[:, pl.ds(2, 4), :], local.at[4])
    own_rows.start()
    small = [
        pltpu.make_async_copy(src, dst, local.at[6 + i])
        for i, (src, dst) in enumerate(
            ((spec_in, spec), (wn_in, wn), (quad_in, quad), (kin_in, kin), (pho_in, pho), (hw_in, hw))
        )
    ]
    for copy in small:
        copy.start()

    barrier = pltpu.get_barrier_semaphore()

    def hello(dw, dl, dg):
        pl.semaphore_signal(barrier, inc=1, device_id=(dw, dl, dg), device_id_type=MESH)

    for k in FAR_W:
        hello(lax.rem(w + k, NW), l, g)
    for k in range(NL):
        ll = lax.rem(l + k, NL)
        hello(up_w, ll, up_g)
        hello(down_w, ll, down_g)
        if k:
            hello(w, ll, g)
    for k in FAR_G:
        hello(w, l, lax.rem(g + k, NG))
    count = (NW - 1) + (NG - 1) + (NL - 1) + 2 * NL

    for row in (0, 7):
        PH[pl.ds(row, 1), :] = jnp.zeros((1, NLON), F32)

    small[0].wait()
    small[1].wait()
    own_wave = wn[pos]
    for p in range(2):
        for f in range(4):
            X[pl.ds(4 * p + f, 1), :] = spec[p, 0, 0, pl.ds(f, 1), :].astype(F32)
    degree = lax.broadcasted_iota(jnp.int32, (8, NDEG), 1)
    coeffs = jnp.where(degree < NDEG - own_wave, X[...], 0.0).astype(BF16)
    fourier = jnp.zeros((8, NLAT), F32)
    for i in range(4):
        rows = pl.ds(256 * i, 256)
        pltpu.make_async_copy(leg.at[0, rows, :], LV.at[rows, :], local.at[i]).wait()
        fourier += jnp.dot(
            coeffs[:, 256 * i : 256 * i + 256], LV[rows, :], preferred_element_type=F32
        )
    groups = []
    for c in range(2):
        for r in range(8):
            shift = (NLAT - (4 * c + r - 2)) % NLAT
            groups.append(pltpu.roll(fourier, shift, 1) if shift else fourier)
    T[...] = jnp.concatenate(groups, axis=0).T
    S[...] = T[pl.ds(0, 48, stride=8), :].reshape(NW, 4, 128)
    own_rows.wait()

    pl.semaphore_wait(barrier, count)

    def z_copy(src, dst, ssem, rsem, k):
        there = lax.rem(w + k, NW)
        return pltpu.make_async_remote_copy(
            src.at[there], dst.at[w], ssem.at[k], rsem.at[w],
            device_id=(there, l, g), device_id_type=MESH,
        )

    def z_arrival(src, dst, ssem, rsem, k):
        there = lax.rem(w + k, NW)
        return pltpu.make_async_remote_copy(
            src.at[there], dst.at[there], ssem.at[k], rsem.at[there],
            device_id=(there, l, g), device_id_type=MESH,
        )

    def g_copy(src, dst, ssem, rsem, k, share):
        there = lax.rem(g + k, NG)
        return pltpu.make_async_remote_copy(
            src.at[:, there // share, :], dst.at[:, g, :], ssem.at[k], rsem.at[g],
            device_id=(w, l, there), device_id_type=MESH,
        )

    def g_arrival(src, dst, ssem, rsem, k, share):
        there = lax.rem(g + k, NG)
        return pltpu.make_async_remote_copy(
            src.at[:, there // share, :], dst.at[:, there, :], ssem.at[k], rsem.at[there],
            device_id=(w, l, there), device_id_type=MESH,
        )

    def l_copy(k, arrival=False):
        there = lax.rem(l + k, NL)
        return pltpu.make_async_remote_copy(
            C.at[0, pl.ds(2, 4), pl.ds(pl.multiple_of(CHUNK * there, CHUNK), CHUNK)],
            LR.at[there if arrival else l], ls.at[k], lr.at[there if arrival else l],
            device_id=(w, there, g), device_id_type=MESH,
        )

    def p_copy(k, arrival=False):
        there = lax.rem(l + k, NL)
        part = there if arrival else l
        return pltpu.make_async_remote_copy(
            PC.at[there],
            PH.at[pl.ds(2, 4), pl.ds(pl.multiple_of(CHUNK * part, CHUNK), CHUNK)],
            ps.at[k], pr.at[part],
            device_id=(w, there, g), device_id_type=MESH,
        )

    def e_copy(side, k, arrival=False):
        there = lax.rem(l + k, NL)
        part = there if arrival else l
        return pltpu.make_async_remote_copy(
            PC.at[there, pl.ds(3 if side else 0, 1)],
            PH.at[pl.ds(1 if side else 6, 1), pl.ds(pl.multiple_of(CHUNK * part, CHUNK), CHUNK)],
            es.at[side, k], er.at[side, part],
            device_id=(up_w, there, up_g) if side else (down_w, there, down_g),
            device_id_type=MESH,
        )

    def h_copy(side):
        return pltpu.make_async_remote_copy(
            C.at[:, pl.ds(4 if side else 2, 2), :],
            C.at[:, pl.ds(0 if side else 6, 2), :],
            hs.at[side], hr.at[side],
            device_id=(up_w, l, up_g) if side else (down_w, l, down_g),
            device_id_type=MESH,
        )

    for k in FAR_W:
        z_copy(S, Z1, zs, zr, k).start()
    for k in FAR_L:
        l_copy(k).start()
    for side in range(2):
        h_copy(side).start()
    Z1[w] = S[w]
    LR[l] = C[0, pl.ds(2, 4), pl.ds(pl.multiple_of(CHUNK * l, CHUNK), CHUNK)]

    for s in range(NPOS):
        WC[pl.ds(s, 1), :] = jnp.full((1, 128), wn[s], jnp.int32)
    WC[pl.ds(NPOS, 128 - NPOS), :] = jnp.zeros((128 - NPOS, 128), jnp.int32)
    waves = WC[...]
    across = waves.astype(F32).T[:16, :].astype(jnp.int32)
    coarse = lax.broadcasted_iota(jnp.int32, (16, 128), 0) * 256
    AT[0], AT[1] = cos_sin((across * coarse) & (NLON - 1))
    used = lax.broadcasted_iota(jnp.int32, (128, 128), 0) < NPOS
    for half in range(2):
        fine = lax.broadcasted_iota(jnp.int32, (128, 128), 1) + 128 * half
        cos, sin = cos_sin((waves * fine) & (NLON - 1))
        for p, table in enumerate((cos, -sin)):
            hi, lo = split(jnp.where(used, table, 0.0))
            BH[pl.ds(128 * p, 128), pl.ds(128 * half, 128)] = hi
            BL[pl.ds(128 * p, 128), pl.ds(128 * half, 128)] = lo

    for k in range(1, NL):
        l_copy(k, True).wait_recv()
    total = jnp.zeros((4, CHUNK), F32)
    for level in range(NL):
        PC[level] = 0.2 * jnp.exp(total * (-2.0 / NL))
        if level < NL - 1:
            total += LR[level]
    for k in FAR_L:
        p_copy(k).start()
    for k in range(NL):
        for side in range(2):
            e_copy(side, k).start()
    PH[pl.ds(2, 4), pl.ds(pl.multiple_of(CHUNK * l, CHUNK), CHUNK)] = PC[l]

    for k in range(1, NW):
        z_arrival(S, Z1, zs, zr, k).wait_recv()
    for k in FAR_G:
        g_copy(Z1, G1, gs, gr, k, 2).start()
    G1[:, pl.ds(g, 1), :] = Z1[:, pl.ds(g // 2, 1), :]

    for side in range(2):
        h_copy(side).wait_recv()

    @pl.when(pos == 0)
    def _():
        C[:, pl.ds(0, 2), :] = jnp.zeros((8, 2, NLON), F32)

    @pl.when(pos == NPOS - 1)
    def _():
        C[:, pl.ds(6, 2), :] = jnp.zeros((8, 2, NLON), F32)

    for k in range(1, NG):
        g_arrival(Z1, G1, gs, gr, k, 2).wait_recv()

    arrived = jnp.concatenate([G1[...].reshape(NPOS, 128), jnp.zeros((128 - NPOS, 128), F32)], axis=0)
    V[...] = arrived.T
    second = lax.rem(g, 2) == 1
    parts = []
    for p in range(2):
        fields = []
        for f in range(4):
            first = V[pl.ds(4 * p + f, 8, stride=8), :]
            other = V[pl.ds(64 + 4 * p + f, 8, stride=8), :]
            fields.append(jnp.where(second, other, first))
        parts.append(jnp.concatenate(fields, axis=0) * (1.0 / math.sqrt(NPOS)))
    real, imag = parts
    latitude = lax.broadcasted_iota(jnp.int32, (8, 256), 0) + (4 * pos - 2)
    inside = jnp.where((latitude >= 0) & (latitude < NLAT), 1.0, 0.0)
    bh, bl = BH[...], BL[...]
    for part in range(4):
        turned = []
        for i in range(4):
            h = 4 * part + i
            ca, sa = AT[0, pl.ds(h, 1), :], AT[1, pl.ds(h, 1), :]
            turned.append(
                jnp.concatenate([real * ca - imag * sa, real * sa + imag * ca], axis=1)
            )
        grid = dot3(jnp.concatenate(turned, axis=0), bh, bl, (((1,), (0,)), ((), ())))
        for i in range(4):
            cols = pl.ds(256 * (4 * part + i), 256)
            field = [grid[32 * i + 8 * f : 32 * i + 8 * f + 8, :] for f in range(4)]
            cx = 0.45 * jnp.tanh(field[0]) * inside
            cy = 0.45 * jnp.tanh(field[1]) * inside
            COEF[0, :, cols] = inside - jnp.abs(cx) - jnp.abs(cy)
            COEF[1, :, cols] = jnp.maximum(cx, 0.0)
            COEF[2, :, cols] = jnp.maximum(-cx, 0.0)
            COEF[3, :, cols] = jnp.maximum(cy, 0.0)
            COEF[4, :, cols] = jnp.maximum(-cy, 0.0)
            COEF[5, :, cols] = 0.2 * jnp.exp(0.3 * field[2])
            COEF[6, :, cols] = 1.0 + 0.5 * jnp.tanh(field[3])

    for copy in small[2:]:
        copy.wait()
    lane = lax.broadcasted_iota(jnp.int32, (8, 128), 1)

    def transported(here, pick):
        b = here // 128
        west = pl.ds(pl.multiple_of(lax.rem(b + 31, 32) * 128, 128), 128)
        east = pl.ds(pl.multiple_of(lax.rem(b + 1, 32) * 128, 128), 128)
        here = pl.ds(pl.multiple_of(here, 128), 128)
        cc, xp, xm, yp, ym = [COEF[i, :, here] for i in range(5)]

        def of(t):
            c = pick(t, here)
            western = pltpu.roll(jnp.where(lane == 127, pick(t, west), c), 1, 1)
            eastern = pltpu.roll(jnp.where(lane == 0, pick(t, east), c), 127, 1)
            northern = pltpu.roll(c, 1, 0)
            southern = pltpu.roll(c, 7, 0)
            return cc * c + xp * western + xm * eastern + yp * northern + ym * southern

        return of

    def transport(src, dst):
        def block(b, carry):
            of = transported(b * 128, lambda t, cols: src[t, :, cols])
            for t in range(8):
                dst[t, :, pl.ds(pl.multiple_of(b * 128, 128), 128)] = of(t)
            return carry

        lax.fori_loop(0, 32, block, 0, unroll=8)

    def mix(src, dst, heats):
        def block(b, carry):
            cols = pl.ds(pl.multiple_of(b * 512, 512), 512)
            rate = COEF[5, :, cols]
            moved = [src[t, :, cols] for t in range(8)]
            heat = [None] * 3
            for i in range(8):
                mixed = kin[i, 0] * moved[0]
                for t in range(1, 8):
                    mixed += kin[i, t] * moved[t]
                done = moved[i] + rate * mixed
                dst[i, :, cols] = done
                if heats:
                    heat = [
                        hw[k, i] * done if old is None else old + hw[k, i] * done
                        for k, old in enumerate(heat)
                    ]
            if heats:
                for k in range(3):
                    HN[k, :, cols] = heat[k]
            return carry

        lax.fori_loop(0, 8, block, 0)

    transport(C, M)
    mix(M, D, False)
    transport(D, O)
    mix(O, D, True)
    for i in range(8):
        total = jnp.full((8, 128), kin[i, 0] * pho[0], F32)
        for t in range(1, 8):
            total += jnp.full((8, 128), kin[i, t] * pho[t], F32)
        KP[i] = total
    for k in range(3):
        first = jnp.full((8, 128), hw[k, 0] * pho[0], F32)
        second = hw[k, 0] * KP[0]
        for t in range(1, 8):
            first += jnp.full((8, 128), hw[k, t] * pho[t], F32)
            second += hw[k, t] * KP[t]
        KP[8 + k] = first
        KP[11 + k] = second

    for k in range(NL):
        if k:
            p_copy(k, True).wait_recv()
        for side in range(2):
            e_copy(side, k, True).wait_recv()
    Q[...] = PH[...] * M[0]

    def finish(b, carry):
        here = pl.ds(pl.multiple_of(b * 128, 128), 128)
        lit = transported(b * 128, lambda t, cols: Q[:, cols])(0)
        both = lit + PH[:, here] * (O[0, :, here] + pho[0] * lit)
        late = COEF[5, :, here] * lit
        for i in range(8):
            done = D[i, :, here] + (pho[i] * both + KP[i] * late)
            tout[i, 0, :, here] = done[2:6, :]
        gain = COEF[6, :, here]
        for k in range(3):
            H[b, pl.ds(8 * k, 8), :] = (HN[k, :, here] + (KP[8 + k] * both + KP[11 + k] * late)) * gain
        return carry

    lax.fori_loop(0, 32, finish, 0, unroll=4)

    zr_sum = jnp.zeros((24, 128), F32)
    zi_sum = jnp.zeros((24, 128), F32)
    for part in range(4):
        rows = []
        for i in range(4):
            h = 4 * part + i
            rows.append(jnp.concatenate([H[2 * h], H[2 * h + 1]], axis=1))
        spectrum = dot3(jnp.concatenate(rows, axis=0), bh, bl, NT)
        for i in range(4):
            h = 4 * part + i
            ca, sa = AT[0, pl.ds(h, 1), :], AT[1, pl.ds(h, 1), :]
            yc = spectrum[24 * i : 24 * i + 24, :128]
            ys = spectrum[24 * i : 24 * i + 24, 128:]
            zr_sum += ca * yc + sa * ys
            zi_sum += ca * ys - sa * yc
    scale = 1.0 / math.sqrt(NLON)
    HF[pl.ds(0, 24), :] = zr_sum * scale
    HF[pl.ds(24, 24), :] = zi_sum * scale
    HF[pl.ds(48, 16), :] = jnp.zeros((16, 128), F32)
    mine = jnp.concatenate([HF[pl.ds(r, 8, stride=8), :] for r in range(2, 6)], axis=0)
    S2[:, pl.ds(0, 32)] = mine.T

    def back(dw, dg):
        there_w, there_g = lax.rem(w + dw, NW), lax.rem(g + dg, NG)
        return pltpu.make_async_remote_copy(
            S2.at[pl.ds(there_w * NG + there_g, 1), LANES], G2.at[pl.ds(pos, 1), LANES],
            zs2.at[0], zr2.at[0],
            device_id=(there_w, l, there_g), device_id_type=MESH,
        )

    for dw, dg in PEERS:
        back(dw, dg).start()
    G2[pl.ds(pos, 1), :] = S2[pl.ds(pos, 1), :]
    every = pltpu.make_async_remote_copy(
        S2.at[pl.ds(0, NPOS - 1), LANES], G2.at[pl.ds(0, NPOS - 1), LANES], zs2.at[0], zr2.at[0],
        device_id=(up_w, l, up_g), device_id_type=MESH,
    )
    every.wait_recv()

    bands = G2[...]
    for r in range(4):
        WT[pl.ds(r, NPOS, stride=4), :] = pltpu.roll(bands, 128 - 8 * r, 1) if r else bands
    weighted = (WT[...].T[:8, :] * quad[...].reshape(1, NLAT)).astype(BF16)
    found = lax.dot_general(weighted, LV[...], NT, preferred_element_type=F32)
    found = jnp.where(degree < NDEG - own_wave, found, 0.0)
    for p in range(2):
        for k in range(3):
            sout[p, k, 0] = found[3 * p + k : 3 * p + k + 1, :]

    every.wait_send()
    for k in range(1, NW):
        z_copy(S, Z1, zs, zr, k).wait_send()
    for k in range(1, NG):
        g_copy(Z1, G1, gs, gr, k, 2).wait_send()
    for k in range(NL):
        if k:
            l_copy(k).wait_send()
            p_copy(k).wait_send()
        for side in range(2):
            e_copy(side, k).wait_send()
    for side in range(2):
        h_copy(side).wait_send()


def body(spectra, legendre, wavenumbers, quad_weights, tracers, kinetics, photolysis, heat_weights):
    vmem = pl.BlockSpec(memory_space=pltpu.VMEM)
    hbm = pl.BlockSpec(memory_space=pl.ANY)
    V, DMA = pltpu.VMEM, pltpu.SemaphoreType.DMA
    return pl.pallas_call(
        kernel,
        out_shape=(
            V((8, 1, 4, NLON), F32),
            V((2, 3, 1, 1, NDEG), F32),
        ),
        in_specs=[hbm] * 8,
        out_specs=(vmem, vmem),
        scratch_shapes=[
            V((2, 1, 1, 4, NDEG), BF16), pltpu.SMEM((NPOS,), jnp.int32), V((NLAT,), F32),
            pltpu.SMEM((8, 8), F32), pltpu.SMEM((8,), F32), pltpu.SMEM((3, 8), F32),
            V((8, 8, NLON), F32), V((8, 8, NLON), F32), V((8, 8, NLON), F32), V((8, 8, NLON), F32),
            V((8, NLON), F32), V((3, 8, NLON), F32), V((14, 8, 128), F32),
            V((NDEG, NLAT), BF16), V((8, NDEG), F32),
            V((NLAT, 128), F32), V((NW, 4, 128), F32), V((NW, 4, 128), F32), V((NW, NG, 128), F32),
            V((128, 128), F32),
            V((NL, 4, CHUNK), F32), V((NL, 4, CHUNK), F32), V((8, NLON), F32),
            V((7, 8, NLON), F32),
            V((2, 16, 128), F32), V((256, 256), BF16), V((256, 256), BF16),
            V((32, 24, 128), F32), V((64, 128), F32),
            V((128, 128), F32), V((NPOS, 128), F32),
            V((NLAT, 128), F32), V((128, 128), jnp.int32),
            DMA((12,)), DMA((NW,)), DMA((NW,)), DMA((NG,)), DMA((NG,)), DMA((NL,)), DMA((NL,)),
            DMA((NL,)), DMA((NL,)), DMA((2, NL)), DMA((2, NL)), DMA((2,)), DMA((2,)),
            DMA((1,)), DMA((1,)),
        ],
        compiler_params=pltpu.CompilerParams(collective_id=0, has_side_effects=True),
    )(
        spectra.transpose(0, 2, 3, 1, 4), legendre, wavenumbers, quad_weights, tracers, kinetics,
        photolysis, heat_weights,
    )


def solution(mesh):
    return jax.shard_map(
        body,
        mesh=mesh,
        in_specs=(
            P(None, None, "lev", ("wave", "grp"), None),
            P(("wave", "grp"), None, None),
            P(),
            P(),
            P(None, "lev", ("wave", "grp"), None),
            P(),
            P(),
            P(),
        ),
        out_specs=(
            P(None, "lev", ("wave", "grp"), None),
            P(None, None, "lev", ("wave", "grp"), None),
        ),
        check_vma=False,
    )
```

```python
import math

import jax
import jax.numpy as jnp
from jax import lax
from jax.experimental import pallas as pl
from jax.experimental.pallas import tpu as pltpu
from jax.sharding import PartitionSpec as P

NW, NL, NG = 12, 8, 8
NPOS = NW * NG
NDEG = 1024
NLON = 4096
NLAT = 384
CHUNK = NLON // NL
F32 = jnp.float32
BF16 = jnp.bfloat16
MESH = pl.DeviceIdType.MESH
NT = (((1,), (1,)), ((), ()))
FAR_L = (4, 3, 5, 2, 6, 1, 7)


def wrapped(i, n):
    return jnp.where(i >= n, i - n, i)


def outward(i, n):
    return n // 2 + ((i + 1) >> 1) * (1 - 2 * (i & 1))


def each_peer(w, g, act):
    def row(i, carry):
        for j in range(NG):
            act(wrapped(w + outward(i, NW), NW), wrapped(g + outward(j, NG), NG))
        return carry

    lax.fori_loop(0, NW - 1, row, 0)
    for j in range(NG - 1):
        act(w, wrapped(g + outward(j, NG), NG))


def cos_sin(m):
    shifted = m + NLON // 8
    quarter = (shifted >> 10) & 3
    angle = ((shifted & (NLON // 4 - 1)) - NLON // 8).astype(F32) * (2.0 * math.pi / NLON)
    z = angle * angle
    s = angle * (1.0 + z * (-1.0 / 6 + z * (1.0 / 120 + z * (-1.0 / 5040 + z * (1.0 / 362880)))))
    c = 1.0 + z * (-0.5 + z * (1.0 / 24 + z * (-1.0 / 720 + z * (1.0 / 40320))))
    odd = (quarter & 1) == 1
    cos = jnp.where(odd, s, c)
    sin = jnp.where(odd, c, s)
    cos = jnp.where(((quarter + 1) & 2) == 2, -cos, cos)
    sin = jnp.where((quarter & 2) == 2, -sin, sin)
    return cos, sin


def split(x):
    hi = x.astype(BF16)
    return hi, (x - hi.astype(F32)).astype(BF16)


def dot3(x, bh, bl, dims):
    hi, lo = split(x)
    out = lax.dot_general(hi, bh, dims, preferred_element_type=F32)
    out += lax.dot_general(lo, bh, dims, preferred_element_type=F32)
    return out + lax.dot_general(hi, bl, dims, preferred_element_type=F32)


def kernel(
    spec_in, leg, wn_in, quad_in, trc, kin_in, pho_in, hw_in,
    tout, sout,
    spec, wn, quad, kin, pho, hw, C, D, O, M, Q, HN, KP, LV, X, T, G1, V, LR, PC, PH, COEF, AT, BH, BL, H, HF, S2, G2, WT, WC,
    local, gs, gr, ls, lr, ps, pr, es, er, hs, hr, gs2, gr2,
):
    w = lax.axis_index("wave")
    l = lax.axis_index("lev")
    g = lax.axis_index("grp")
    pos = w * NG + g
    up = lax.rem(pos + 1, NPOS)
    down = lax.rem(pos + NPOS - 1, NPOS)
    up_w, up_g = up // NG, lax.rem(up, NG)
    down_w, down_g = down // NG, lax.rem(down, NG)

    for i in range(4):
        rows = pl.ds(256 * i, 256)
        pltpu.make_async_copy(leg.at[0, rows, :], LV.at[rows, :], local.at[i]).start()
    own_rows = pltpu.make_async_copy(trc.at[:, 0], C.at[:, pl.ds(2, 4), :], local.at[4])
    own_rows.start()
    small = [
        pltpu.make_async_copy(src, dst, local.at[6 + i])
        for i, (src, dst) in enumerate(
            ((spec_in, spec), (wn_in, wn), (quad_in, quad), (kin_in, kin), (pho_in, pho), (hw_in, hw))
        )
    ]
    for copy in small:
        copy.start()

    barrier = pltpu.get_barrier_semaphore()

    def hello(dw, dl, dg):
        pl.semaphore_signal(barrier, inc=1, device_id=(dw, dl, dg), device_id_type=MESH)

    each_peer(w, g, lambda dw, dg: hello(dw, l, dg))
    for k in FAR_L:
        ll = wrapped(l + k, NL)
        hello(up_w, ll, up_g)
        hello(down_w, ll, down_g)
        hello(w, ll, g)
    count = NPOS - 1 + 3 * (NL - 1)

    for row in (0, 7):
        PH[pl.ds(row, 1), :] = jnp.zeros((1, NLON), F32)

    small[0].wait()
    small[1].wait()
    own_wave = wn[pos]
    for p in range(2):
        for f in range(4):
            X[pl.ds(4 * p + f, 1), :] = spec[p, 0, 0, pl.ds(f, 1), :].astype(F32)
    degree = lax.broadcasted_iota(jnp.int32, (8, NDEG), 1)
    coeffs = jnp.where(degree < NDEG - own_wave, X[...], 0.0).astype(BF16)
    fourier = jnp.zeros((8, NLAT), F32)
    for i in range(4):
        rows = pl.ds(256 * i, 256)
        pltpu.make_async_copy(leg.at[0, rows, :], LV.at[rows, :], local.at[i]).wait()
        fourier += jnp.dot(
            coeffs[:, 256 * i : 256 * i + 256], LV[rows, :], preferred_element_type=F32
        )
    groups = []
    for r in range(8):
        shift = (NLAT + 2 - r) % NLAT
        groups.append(pltpu.roll(fourier, shift, 1) if shift else fourier)
    T[:, pl.ds(0, 64)] = jnp.concatenate(groups, axis=0).T
    own_rows.wait()

    pl.semaphore_wait(barrier, count)

    def send(src, stride, dst, ssem, rsem):
        def act(there_w, there_g):
            pltpu.make_async_remote_copy(
                src.at[pl.ds((there_w * NG + there_g) * stride, 1)], dst.at[pl.ds(pos, 1)],
                ssem.at[0], rsem.at[0],
                device_id=(there_w, l, there_g), device_id_type=MESH,
            ).start()

        each_peer(w, g, act)
        dst[pl.ds(pos, 1), :] = src[pl.ds(pos * stride, 1), :]

    def every(src, dst, ssem, rsem):
        rows = pl.ds(0, NPOS - 1)
        return pltpu.make_async_remote_copy(
            src.at[rows], dst.at[rows], ssem.at[0], rsem.at[0],
            device_id=(up_w, l, up_g), device_id_type=MESH,
        )

    def l_copy(k, arrival=False):
        there = lax.rem(l + k, NL)
        return pltpu.make_async_remote_copy(
            C.at[0, pl.ds(2, 4), pl.ds(pl.multiple_of(CHUNK * there, CHUNK), CHUNK)],
            LR.at[there if arrival else l], ls.at[k], lr.at[there if arrival else l],
            device_id=(w, there, g), device_id_type=MESH,
        )

    def p_copy(k, arrival=False):
        there = lax.rem(l + k, NL)
        part = there if arrival else l
        return pltpu.make_async_remote_copy(
            PC.at[there],
            PH.at[pl.ds(2, 4), pl.ds(pl.multiple_of(CHUNK * part, CHUNK), CHUNK)],
            ps.at[k], pr.at[part],
            device_id=(w, there, g), device_id_type=MESH,
        )

    def e_copy(side, k, arrival=False):
        there = lax.rem(l + k, NL)
        part = there if arrival else l
        return pltpu.make_async_remote_copy(
            PC.at[there, pl.ds(3 if side else 0, 1)],
            PH.at[pl.ds(1 if side else 6, 1), pl.ds(pl.multiple_of(CHUNK * part, CHUNK), CHUNK)],
            es.at[side, k], er.at[side, part],
            device_id=(up_w, there, up_g) if side else (down_w, there, down_g),
            device_id_type=MESH,
        )

    def h_copy(side):
        return pltpu.make_async_remote_copy(
            C.at[:, pl.ds(4 if side else 2, 2), :],
            C.at[:, pl.ds(0 if side else 6, 2), :],
            hs.at[side], hr.at[side],
            device_id=(up_w, l, up_g) if side else (down_w, l, down_g),
            device_id_type=MESH,
        )

    send(T, 4, G1, gs, gr)
    for k in FAR_L:
        l_copy(k).start()
    for side in range(2):
        h_copy(side).start()
    LR[l] = C[0, pl.ds(2, 4), pl.ds(pl.multiple_of(CHUNK * l, CHUNK), CHUNK)]

    for s in range(NPOS):
        WC[pl.ds(s, 1), :] = jnp.full((1, 128), wn[s], jnp.int32)
    WC[pl.ds(NPOS, 128 - NPOS), :] = jnp.zeros((128 - NPOS, 128), jnp.int32)
    waves = WC[...]
    across = waves.astype(F32).T[:16, :].astype(jnp.int32)
    coarse = lax.broadcasted_iota(jnp.int32, (16, 128), 0) * 256
    AT[0], AT[1] = cos_sin((across * coarse) & (NLON - 1))
    used = lax.broadcasted_iota(jnp.int32, (128, 128), 0) < NPOS
    for half in range(2):
        fine = lax.broadcasted_iota(jnp.int32, (128, 128), 1) + 128 * half
        cos, sin = cos_sin((waves * fine) & (NLON - 1))
        for p, table in enumerate((cos, -sin)):
            hi, lo = split(jnp.where(used, table, 0.0))
            BH[pl.ds(128 * p, 128), pl.ds(128 * half, 128)] = hi
            BL[pl.ds(128 * p, 128), pl.ds(128 * half, 128)] = lo

    for k in range(1, NL):
        l_copy(k, True).wait_recv()
    total = jnp.zeros((4, CHUNK), F32)
    for level in range(NL):
        PC[level] = 0.2 * jnp.exp(total * (-2.0 / NL))
        if level < NL - 1:
            total += LR[level]
    for k in FAR_L:
        p_copy(k).start()
    for k in range(NL):
        for side in range(2):
            e_copy(side, k).start()
    PH[pl.ds(2, 4), pl.ds(pl.multiple_of(CHUNK * l, CHUNK), CHUNK)] = PC[l]

    for side in range(2):
        h_copy(side).wait_recv()

    @pl.when(pos == 0)
    def _():
        C[:, pl.ds(0, 2), :] = jnp.zeros((8, 2, NLON), F32)

    @pl.when(pos == NPOS - 1)
    def _():
        C[:, pl.ds(6, 2), :] = jnp.zeros((8, 2, NLON), F32)

    every(T, G1, gs, gr).wait_recv()

    arrived = jnp.concatenate([G1[...], jnp.zeros((128 - NPOS, 128), F32)], axis=0)
    V[...] = arrived.T
    parts = []
    for p in range(2):
        fields = [V[pl.ds(4 * p + f, 8, stride=8), :] for f in range(4)]
        parts.append(jnp.concatenate(fields, axis=0) * (1.0 / math.sqrt(NPOS)))
    real, imag = parts
    latitude = lax.broadcasted_iota(jnp.int32, (8, 256), 0) + (4 * pos - 2)
    inside = jnp.where((latitude >= 0) & (latitude < NLAT), 1.0, 0.0)
    bh, bl = BH[...], BL[...]
    for part in range(4):
        turned = []
        for i in range(4):
            h = 4 * part + i
            ca, sa = AT[0, pl.ds(h, 1), :], AT[1, pl.ds(h, 1), :]
            turned.append(
                jnp.concatenate([real * ca - imag * sa, real * sa + imag * ca], axis=1)
            )
        grid = dot3(jnp.concatenate(turned, axis=0), bh, bl, (((1,), (0,)), ((), ())))
        for i in range(4):
            cols = pl.ds(256 * (4 * part + i), 256)
            field = [grid[32 * i + 8 * f : 32 * i + 8 * f + 8, :] for f in range(4)]
            cx = 0.45 * jnp.tanh(field[0]) * inside
            cy = 0.45 * jnp.tanh(field[1]) * inside
            COEF[0, :, cols] = inside - jnp.abs(cx) - jnp.abs(cy)
            COEF[1, :, cols] = jnp.maximum(cx, 0.0)
            COEF[2, :, cols] = jnp.maximum(-cx, 0.0)
            COEF[3, :, cols] = jnp.maximum(cy, 0.0)
            COEF[4, :, cols] = jnp.maximum(-cy, 0.0)
            COEF[5, :, cols] = 0.2 * jnp.exp(0.3 * field[2])
            COEF[6, :, cols] = 1.0 + 0.5 * jnp.tanh(field[3])

    for copy in small[2:]:
        copy.wait()
    lane = lax.broadcasted_iota(jnp.int32, (8, 128), 1)

    def transported(b, pick):
        west = pl.ds(pl.multiple_of(((b + 31) & 31) * 128, 128), 128)
        east = pl.ds(pl.multiple_of(((b + 1) & 31) * 128, 128), 128)
        here = pl.ds(pl.multiple_of(b * 128, 128), 128)
        cc, xp, xm, yp, ym = [COEF[i, :, here] for i in range(5)]

        def of(t):
            c = pick(t, here)
            western = pltpu.roll(jnp.where(lane == 127, pick(t, west), c), 1, 1)
            eastern = pltpu.roll(jnp.where(lane == 0, pick(t, east), c), 127, 1)
            northern = pltpu.roll(c, 1, 0)
            southern = pltpu.roll(c, 7, 0)
            return cc * c + xp * western + xm * eastern + yp * northern + ym * southern

        return of

    def transport(src, dst):
        def block(b, carry):
            of = transported(b, lambda t, cols: src[t, :, cols])
            for t in range(8):
                dst[t, :, pl.ds(pl.multiple_of(b * 128, 128), 128)] = of(t)
            return carry

        lax.fori_loop(0, 32, block, 0, unroll=16)

    def mix(src, dst, heats):
        def block(b, carry):
            cols = pl.ds(pl.multiple_of(b * 512, 512), 512)
            rate = COEF[5, :, cols]
            moved = [src[t, :, cols] for t in range(8)]
            heat = [None] * 3
            for i in range(8):
                mixed = kin[i, 0] * moved[0]
                for t in range(1, 8):
                    mixed += kin[i, t] * moved[t]
                done = moved[i] + rate * mixed
                dst[i, :, cols] = done
                if heats:
                    heat = [
                        hw[k, i] * done if old is None else old + hw[k, i] * done
                        for k, old in enumerate(heat)
                    ]
            if heats:
                for k in range(3):
                    HN[k, :, cols] = heat[k]
            return carry

        lax.fori_loop(0, 8, block, 0)

    transport(C, M)
    mix(M, D, False)
    transport(D, O)
    mix(O, D, True)
    for i in range(8):
        total = jnp.full((8, 128), kin[i, 0] * pho[0], F32)
        for t in range(1, 8):
            total += jnp.full((8, 128), kin[i, t] * pho[t], F32)
        KP[i] = total
    for k in range(3):
        first = jnp.full((8, 128), hw[k, 0] * pho[0], F32)
        second = hw[k, 0] * KP[0]
        for t in range(1, 8):
            first += jnp.full((8, 128), hw[k, t] * pho[t], F32)
            second += hw[k, t] * KP[t]
        KP[8 + k] = first
        KP[11 + k] = second

    for k in range(NL):
        if k:
            p_copy(k, True).wait_recv()
        for side in range(2):
            e_copy(side, k, True).wait_recv()
    Q[...] = PH[...] * M[0]

    def finish(b, carry):
        here = pl.ds(pl.multiple_of(b * 128, 128), 128)
        lit = transported(b, lambda t, cols: Q[:, cols])(0)
        both = lit + PH[:, here] * (O[0, :, here] + pho[0] * lit)
        late = COEF[5, :, here] * lit
        for i in range(8):
            done = D[i, :, here] + (pho[i] * both + KP[i] * late)
            tout[i, 0, :, here] = done[2:6, :]
        gain = COEF[6, :, here]
        for k in range(3):
            H[b, pl.ds(8 * k, 8), :] = (HN[k, :, here] + (KP[8 + k] * both + KP[11 + k] * late)) * gain
        return carry

    lax.fori_loop(0, 32, finish, 0, unroll=4)

    zr_sum = jnp.zeros((24, 128), F32)
    zi_sum = jnp.zeros((24, 128), F32)
    for part in range(4):
        rows = []
        for i in range(4):
            h = 4 * part + i
            rows.append(jnp.concatenate([H[2 * h], H[2 * h + 1]], axis=1))
        spectrum = dot3(jnp.concatenate(rows, axis=0), bh, bl, NT)
        for i in range(4):
            h = 4 * part + i
            ca, sa = AT[0, pl.ds(h, 1), :], AT[1, pl.ds(h, 1), :]
            yc = spectrum[24 * i : 24 * i + 24, :128]
            ys = spectrum[24 * i : 24 * i + 24, 128:]
            zr_sum += ca * yc + sa * ys
            zi_sum += ca * ys - sa * yc
    scale = 1.0 / math.sqrt(NLON)
    HF[pl.ds(0, 24), :] = zr_sum * scale
    HF[pl.ds(24, 24), :] = zi_sum * scale
    HF[pl.ds(48, 16), :] = jnp.zeros((16, 128), F32)
    mine = jnp.concatenate([HF[pl.ds(r, 8, stride=8), :] for r in range(2, 6)], axis=0)
    S2[:, pl.ds(0, 32)] = mine.T

    send(S2, 1, G2, gs2, gr2)
    every(S2, G2, gs2, gr2).wait_recv()

    bands = G2[...]
    for r in range(4):
        WT[pl.ds(r, NPOS, stride=4), :] = pltpu.roll(bands, 128 - 8 * r, 1) if r else bands
    weighted = (WT[...].T[:8, :] * quad[...].reshape(1, NLAT)).astype(BF16)
    found = lax.dot_general(weighted, LV[...], NT, preferred_element_type=F32)
    found = jnp.where(degree < NDEG - own_wave, found, 0.0)
    for p in range(2):
        for k in range(3):
            sout[p, k, 0] = found[3 * p + k : 3 * p + k + 1, :]

    every(T, G1, gs, gr).wait_send()
    every(S2, G2, gs2, gr2).wait_send()
    for k in range(NL):
        if k:
            l_copy(k).wait_send()
            p_copy(k).wait_send()
        for side in range(2):
            e_copy(side, k).wait_send()
    for side in range(2):
        h_copy(side).wait_send()


def hand_over(tracers_ref, heating_ref, tracers_out, heating_out, sems):
    copies = [
        pltpu.make_async_copy(tracers_ref, tracers_out, sems.at[0]),
        pltpu.make_async_copy(heating_ref, heating_out, sems.at[1]),
    ]
    for copy in copies:
        copy.start()
    for copy in copies:
        copy.wait()


def body(spectra, legendre, wavenumbers, quad_weights, tracers, kinetics, photolysis, heat_weights):
    vmem = pl.BlockSpec(memory_space=pltpu.VMEM)
    hbm = pl.BlockSpec(memory_space=pl.ANY)
    V, DMA = pltpu.VMEM, pltpu.SemaphoreType.DMA
    tracers_out, heating = pl.pallas_call(
        kernel,
        out_shape=(
            V((8, 1, 4, NLON), F32),
            V((2, 3, 1, 1, NDEG), F32),
        ),
        in_specs=[hbm] * 8,
        out_specs=(vmem, vmem),
        scratch_shapes=[
            V((2, 1, 1, 4, NDEG), BF16), pltpu.SMEM((NPOS,), jnp.int32), V((NLAT,), F32),
            pltpu.SMEM((8, 8), F32), pltpu.SMEM((8,), F32), pltpu.SMEM((3, 8), F32),
            V((8, 8, NLON), F32), V((8, 8, NLON), F32), V((8, 8, NLON), F32), V((8, 8, NLON), F32),
            V((8, NLON), F32), V((3, 8, NLON), F32), V((14, 8, 128), F32),
            V((NDEG, NLAT), BF16), V((8, NDEG), F32),
            V((NLAT, 128), F32), V((NPOS, 128), F32),
            V((128, 128), F32),
            V((NL, 4, CHUNK), F32), V((NL, 4, CHUNK), F32), V((8, NLON), F32),
            V((7, 8, NLON), F32),
            V((2, 16, 128), F32), V((256, 256), BF16), V((256, 256), BF16),
            V((32, 24, 128), F32), V((64, 128), F32),
            V((128, 128), F32), V((NPOS, 128), F32),
            V((NLAT, 128), F32), V((128, 128), jnp.int32),
            DMA((12,)), DMA((1,)), DMA((1,)), DMA((NL,)), DMA((NL,)),
            DMA((NL,)), DMA((NL,)), DMA((2, NL)), DMA((2, NL)), DMA((2,)), DMA((2,)),
            DMA((1,)), DMA((1,)),
        ],
        compiler_params=pltpu.CompilerParams(collective_id=0, has_side_effects=True),
    )(
        spectra.transpose(0, 2, 3, 1, 4), legendre, wavenumbers, quad_weights, tracers, kinetics,
        photolysis, heat_weights,
    )
    return pl.pallas_call(
        hand_over,
        out_shape=(
            jax.ShapeDtypeStruct((8, 1, 4, NLON), F32),
            jax.ShapeDtypeStruct((2, 3, 1, 1, NDEG), F32),
        ),
        in_specs=[vmem, vmem],
        out_specs=(hbm, hbm),
        scratch_shapes=[DMA((2,))],
    )(
        pltpu.with_memory_space_constraint(tracers_out, pltpu.VMEM),
        pltpu.with_memory_space_constraint(heating, pltpu.VMEM),
    )


def solution(mesh):
    return jax.shard_map(
        body,
        mesh=mesh,
        in_specs=(
            P(None, None, "lev", ("wave", "grp"), None),
            P(("wave", "grp"), None, None),
            P(),
            P(),
            P(None, "lev", ("wave", "grp"), None),
            P(),
            P(),
            P(),
        ),
        out_specs=(
            P(None, "lev", ("wave", "grp"), None),
            P(None, None, "lev", ("wave", "grp"), None),
        ),
        check_vma=False,
    )
```

```python
import math

import jax
import jax.numpy as jnp
from jax import lax
from jax.experimental import pallas as pl
from jax.experimental.pallas import tpu as pltpu
from jax.sharding import PartitionSpec as P

NW, NL, NG = 12, 8, 8
NPOS = NW * NG
NDEG = 1024
NLON = 4096
NLAT = 384
CHUNK = NLON // NL
F32 = jnp.float32
BF16 = jnp.bfloat16
MESH = pl.DeviceIdType.MESH
NT = (((1,), (1,)), ((), ()))
FAR_L = (4, 3, 5, 2, 6, 1, 7)


def wrapped(i, n):
    return jnp.where(i >= n, i - n, i)


def outward(i, n):
    return n // 2 + ((i + 1) >> 1) * (1 - 2 * (i & 1))


def each_peer(w, g, act):
    def row(i, carry):
        for j in range(NG):
            act(wrapped(w + outward(i, NW), NW), wrapped(g + outward(j, NG), NG))
        return carry

    lax.fori_loop(0, NW - 1, row, 0)
    for j in range(NG - 1):
        act(w, wrapped(g + outward(j, NG), NG))


def cos_sin(m):
    shifted = m + NLON // 8
    quarter = (shifted >> 10) & 3
    angle = ((shifted & (NLON // 4 - 1)) - NLON // 8).astype(F32) * (2.0 * math.pi / NLON)
    z = angle * angle
    s = angle * (1.0 + z * (-1.0 / 6 + z * (1.0 / 120 + z * (-1.0 / 5040 + z * (1.0 / 362880)))))
    c = 1.0 + z * (-0.5 + z * (1.0 / 24 + z * (-1.0 / 720 + z * (1.0 / 40320))))
    odd = (quarter & 1) == 1
    cos = jnp.where(odd, s, c)
    sin = jnp.where(odd, c, s)
    cos = jnp.where(((quarter + 1) & 2) == 2, -cos, cos)
    sin = jnp.where((quarter & 2) == 2, -sin, sin)
    return cos, sin


def split(x):
    hi = x.astype(BF16)
    return hi, (x - hi.astype(F32)).astype(BF16)


def dot3(x, bh, bl, dims):
    hi, lo = split(x)
    out = lax.dot_general(hi, bh, dims, preferred_element_type=F32)
    out += lax.dot_general(lo, bh, dims, preferred_element_type=F32)
    return out + lax.dot_general(hi, bl, dims, preferred_element_type=F32)


def kernel(
    spec_in, leg, wn_in, quad_in, trc, kin_in, pho_in, hw_in,
    tout, sout,
    spec, wn, quad, kin, pho, hw, C, D, O, M, E, Q, HN, KP, CP, AP, LV, X, T, G1, V, LR, PC, PH, COEF, AT, BH, BL, H, HF, S2, G2, WT, WC,
    local, gs, gr, ls, lr, ps, pr, es, er, hs, hr, gs2, gr2,
):
    w = lax.axis_index("wave")
    l = lax.axis_index("lev")
    g = lax.axis_index("grp")
    pos = w * NG + g
    up = lax.rem(pos + 1, NPOS)
    down = lax.rem(pos + NPOS - 1, NPOS)
    up_w, up_g = up // NG, lax.rem(up, NG)
    down_w, down_g = down // NG, lax.rem(down, NG)

    for i in range(4):
        rows = pl.ds(256 * i, 256)
        pltpu.make_async_copy(leg.at[0, rows, :], LV.at[rows, :], local.at[i]).start()
    own_rows = pltpu.make_async_copy(trc.at[:, 0], C.at[:, pl.ds(2, 4), :], local.at[4])
    own_rows.start()
    small = [
        pltpu.make_async_copy(src, dst, local.at[6 + i])
        for i, (src, dst) in enumerate(
            ((spec_in, spec), (wn_in, wn), (quad_in, quad), (kin_in, kin), (pho_in, pho), (hw_in, hw))
        )
    ]
    for copy in small:
        copy.start()

    barrier = pltpu.get_barrier_semaphore()

    def hello(dw, dl, dg):
        pl.semaphore_signal(barrier, inc=1, device_id=(dw, dl, dg), device_id_type=MESH)

    each_peer(w, g, lambda dw, dg: hello(dw, l, dg))
    for k in FAR_L:
        ll = wrapped(l + k, NL)
        hello(up_w, ll, up_g)
        hello(down_w, ll, down_g)
        hello(w, ll, g)
    count = NPOS - 1 + 3 * (NL - 1)

    for row in (0, 7):
        PH[pl.ds(row, 1), :] = jnp.zeros((1, NLON), F32)

    small[0].wait()
    small[1].wait()
    own_wave = wn[pos]
    for p in range(2):
        for f in range(4):
            X[pl.ds(4 * p + f, 1), :] = spec[p, 0, 0, pl.ds(f, 1), :].astype(F32)
    degree = lax.broadcasted_iota(jnp.int32, (8, NDEG), 1)
    coeffs = jnp.where(degree < NDEG - own_wave, X[...], 0.0).astype(BF16)
    fourier = jnp.zeros((8, NLAT), F32)
    for i in range(4):
        rows = pl.ds(256 * i, 256)
        pltpu.make_async_copy(leg.at[0, rows, :], LV.at[rows, :], local.at[i]).wait()
        fourier += jnp.dot(
            coeffs[:, 256 * i : 256 * i + 256], LV[rows, :], preferred_element_type=F32
        )
    groups = []
    for r in range(8):
        shift = (NLAT + 2 - r) % NLAT
        groups.append(pltpu.roll(fourier, shift, 1) if shift else fourier)
    T[:, pl.ds(0, 64)] = jnp.concatenate(groups, axis=0).T
    own_rows.wait()

    pl.semaphore_wait(barrier, count)

    def send(src, stride, dst, ssem, rsem):
        def act(there_w, there_g):
            pltpu.make_async_remote_copy(
                src.at[pl.ds((there_w * NG + there_g) * stride, 1)], dst.at[pl.ds(pos, 1)],
                ssem.at[0], rsem.at[0],
                device_id=(there_w, l, there_g), device_id_type=MESH,
            ).start()

        each_peer(w, g, act)
        dst[pl.ds(pos, 1), :] = src[pl.ds(pos * stride, 1), :]

    def every(src, dst, ssem, rsem):
        rows = pl.ds(0, NPOS - 1)
        return pltpu.make_async_remote_copy(
            src.at[rows], dst.at[rows], ssem.at[0], rsem.at[0],
            device_id=(up_w, l, up_g), device_id_type=MESH,
        )

    def l_copy(k, arrival=False):
        there = lax.rem(l + k, NL)
        return pltpu.make_async_remote_copy(
            C.at[0, pl.ds(2, 4), pl.ds(pl.multiple_of(CHUNK * there, CHUNK), CHUNK)],
            LR.at[there if arrival else l], ls.at[k], lr.at[there if arrival else l],
            device_id=(w, there, g), device_id_type=MESH,
        )

    def p_copy(k, arrival=False):
        there = lax.rem(l + k, NL)
        part = there if arrival else l
        return pltpu.make_async_remote_copy(
            PC.at[there],
            PH.at[pl.ds(2, 4), pl.ds(pl.multiple_of(CHUNK * part, CHUNK), CHUNK)],
            ps.at[k], pr.at[part],
            device_id=(w, there, g), device_id_type=MESH,
        )

    def e_copy(side, k, arrival=False):
        there = lax.rem(l + k, NL)
        part = there if arrival else l
        return pltpu.make_async_remote_copy(
            PC.at[there, pl.ds(3 if side else 0, 1)],
            PH.at[pl.ds(1 if side else 6, 1), pl.ds(pl.multiple_of(CHUNK * part, CHUNK), CHUNK)],
            es.at[side, k], er.at[side, part],
            device_id=(up_w, there, up_g) if side else (down_w, there, down_g),
            device_id_type=MESH,
        )

    def h_copy(side):
        return pltpu.make_async_remote_copy(
            C.at[:, pl.ds(4 if side else 2, 2), :],
            C.at[:, pl.ds(0 if side else 6, 2), :],
            hs.at[side], hr.at[side],
            device_id=(up_w, l, up_g) if side else (down_w, l, down_g),
            device_id_type=MESH,
        )

    send(T, 4, G1, gs, gr)
    for k in FAR_L:
        l_copy(k).start()
    for side in range(2):
        h_copy(side).start()
    LR[l] = C[0, pl.ds(2, 4), pl.ds(pl.multiple_of(CHUNK * l, CHUNK), CHUNK)]

    upper = lax.broadcasted_iota(jnp.int32, (8, 256), 0) < 4

    def packed(first, second):
        return jnp.where(
            upper[:, : first.shape[1]], pltpu.roll(first, 6, 0), pltpu.roll(second, 2, 0)
        )

    for s in range(NPOS):
        WC[pl.ds(s, 1), :] = jnp.full((1, 128), wn[s], jnp.int32)
    WC[pl.ds(NPOS, 128 - NPOS), :] = jnp.zeros((128 - NPOS, 128), jnp.int32)
    waves = WC[...]
    across = waves.astype(F32).T[:16, :].astype(jnp.int32)
    coarse = lax.broadcasted_iota(jnp.int32, (16, 128), 0) * 256
    AT[0], AT[1] = cos_sin((across * coarse) & (NLON - 1))
    for p in range(2):
        for j in range(8):
            low = jnp.broadcast_to(AT[p, pl.ds(j, 1), :], (8, 128))
            high = jnp.broadcast_to(AT[p, pl.ds(j + 8, 1), :], (8, 128))
            AP[p, j] = jnp.where(upper[:, :128], low, high)
    used = lax.broadcasted_iota(jnp.int32, (128, 128), 0) < NPOS
    for half in range(2):
        fine = lax.broadcasted_iota(jnp.int32, (128, 128), 1) + 128 * half
        cos, sin = cos_sin((waves * fine) & (NLON - 1))
        for p, table in enumerate((cos, -sin)):
            hi, lo = split(jnp.where(used, table, 0.0))
            BH[pl.ds(128 * p, 128), pl.ds(128 * half, 128)] = hi
            BL[pl.ds(128 * p, 128), pl.ds(128 * half, 128)] = lo

    for k in range(1, NL):
        l_copy(k, True).wait_recv()
    total = jnp.zeros((4, CHUNK), F32)
    for level in range(NL):
        PC[level] = 0.2 * jnp.exp(total * (-2.0 / NL))
        if level < NL - 1:
            total += LR[level]
    for k in FAR_L:
        p_copy(k).start()
    for k in range(NL):
        for side in range(2):
            e_copy(side, k).start()
    PH[pl.ds(2, 4), pl.ds(pl.multiple_of(CHUNK * l, CHUNK), CHUNK)] = PC[l]

    for copy in small[2:]:
        copy.wait()
    for i in range(8):
        total = jnp.full((8, 128), kin[i, 0] * pho[0], F32)
        for t in range(1, 8):
            total += jnp.full((8, 128), kin[i, t] * pho[t], F32)
        KP[i] = total
    for k in range(3):
        first = jnp.full((8, 128), hw[k, 0] * pho[0], F32)
        second = hw[k, 0] * KP[0]
        for t in range(1, 8):
            first += jnp.full((8, 128), hw[k, t] * pho[t], F32)
            second += hw[k, t] * KP[t]
        KP[8 + k] = first
        KP[11 + k] = second

    for side in range(2):
        h_copy(side).wait_recv()

    @pl.when(pos == 0)
    def _():
        C[:, pl.ds(0, 2), :] = jnp.zeros((8, 2, NLON), F32)

    @pl.when(pos == NPOS - 1)
    def _():
        C[:, pl.ds(6, 2), :] = jnp.zeros((8, 2, NLON), F32)

    every(T, G1, gs, gr).wait_recv()

    arrived = jnp.concatenate([G1[...], jnp.zeros((128 - NPOS, 128), F32)], axis=0)
    V[...] = arrived.T
    parts = []
    for p in range(2):
        fields = [V[pl.ds(4 * p + f, 8, stride=8), :] for f in range(4)]
        parts.append(jnp.concatenate(fields, axis=0) * (1.0 / math.sqrt(NPOS)))
    real, imag = parts
    latitude = lax.broadcasted_iota(jnp.int32, (8, 256), 0) + (4 * pos - 2)
    inside = jnp.where((latitude >= 0) & (latitude < NLAT), 1.0, 0.0)
    bh, bl = BH[...], BL[...]
    for part in range(4):
        blocks = (2 * part, 2 * part + 1, 2 * part + 8, 2 * part + 9)
        turned = []
        for h in blocks:
            ca, sa = AT[0, pl.ds(h, 1), :], AT[1, pl.ds(h, 1), :]
            turned.append(
                jnp.concatenate([real * ca - imag * sa, real * sa + imag * ca], axis=1)
            )
        grid = dot3(jnp.concatenate(turned, axis=0), bh, bl, (((1,), (0,)), ((), ())))
        rates, gains = [], []
        for i, h in enumerate(blocks):
            cols = pl.ds(256 * h, 256)
            field = [grid[32 * i + 8 * f : 32 * i + 8 * f + 8, :] for f in range(4)]
            cx = 0.45 * jnp.tanh(field[0]) * inside
            cy = 0.45 * jnp.tanh(field[1]) * inside
            COEF[0, :, cols] = inside - jnp.abs(cx) - jnp.abs(cy)
            COEF[1, :, cols] = jnp.maximum(cx, 0.0)
            COEF[2, :, cols] = jnp.maximum(-cx, 0.0)
            COEF[3, :, cols] = jnp.maximum(cy, 0.0)
            COEF[4, :, cols] = jnp.maximum(-cy, 0.0)
            rates.append(0.2 * jnp.exp(0.3 * field[2]))
            COEF[5, :, cols] = rates[i]
            gains.append(field[3])
        for i in range(2):
            cols = pl.ds(256 * blocks[i], 256)
            CP[0, :, cols] = packed(rates[i], rates[i + 2])
            CP[1, :, cols] = 1.0 + 0.5 * jnp.tanh(packed(gains[i], gains[i + 2]))

    lane = lax.broadcasted_iota(jnp.int32, (8, 128), 1)

    def transported(b, pick):
        west = pl.ds(pl.multiple_of(((b + 31) & 31) * 128, 128), 128)
        east = pl.ds(pl.multiple_of(((b + 1) & 31) * 128, 128), 128)
        here = pl.ds(pl.multiple_of(b * 128, 128), 128)
        cc, xp, xm, yp, ym = [COEF[i, :, here] for i in range(5)]

        def of(t):
            c = pick(t, here)
            western = pltpu.roll(jnp.where(lane == 127, pick(t, west), c), 1, 1)
            eastern = pltpu.roll(jnp.where(lane == 0, pick(t, east), c), 127, 1)
            northern = pltpu.roll(c, 1, 0)
            southern = pltpu.roll(c, 7, 0)
            return cc * c + xp * western + xm * eastern + yp * northern + ym * southern

        return of

    def transport(b, carry):
        of = transported(b, lambda t, cols: C[t, :, cols])
        for t in range(8):
            M[t, :, pl.ds(pl.multiple_of(b * 128, 128), 128)] = of(t)
        return carry

    def transport_packed(b, carry):
        first = transported(b, lambda t, cols: D[t, :, cols])
        second = transported(b + 16, lambda t, cols: D[t, :, cols])
        for t in range(8):
            O[t, :, pl.ds(pl.multiple_of(b * 128, 128), 128)] = packed(first(t), second(t))
        return carry

    def mix(src, rates, dst, heats):
        def block(b, carry):
            cols = pl.ds(pl.multiple_of(b * 512, 512), 512)
            rate = rates[:, cols]
            moved = [src[t, :, cols] for t in range(8)]
            heat = [None] * 3
            for i in range(8):
                mixed = kin[i, 0] * moved[0]
                for t in range(1, 8):
                    mixed += kin[i, t] * moved[t]
                done = moved[i] + rate * mixed
                dst[i, :, cols] = done
                if heats:
                    heat = [
                        hw[k, i] * done if old is None else old + hw[k, i] * done
                        for k, old in enumerate(heat)
                    ]
            if heats:
                for k in range(3):
                    HN[k, :, cols] = heat[k]
            return carry

        lax.fori_loop(0, dst.shape[2] // 512, block, 0)

    lax.fori_loop(0, 32, transport, 0, unroll=16)
    mix(M, COEF.at[5], D, False)
    lax.fori_loop(0, 16, transport_packed, 0, unroll=8)
    mix(O, CP.at[0], E, True)
    for k in range(NL):
        if k:
            p_copy(k, True).wait_recv()
        for side in range(2):
            e_copy(side, k, True).wait_recv()
    Q[...] = PH[...] * M[0]

    def finish(b, carry):
        here = pl.ds(pl.multiple_of(b * 128, 128), 128)
        there = pl.ds(pl.multiple_of(b * 128 + 2048, 128), 128)
        lit = packed(
            transported(b, lambda t, cols: Q[:, cols])(0),
            transported(b + 16, lambda t, cols: Q[:, cols])(0),
        )
        light = packed(PH[:, here], PH[:, there])
        both = lit + light * (O[0, :, here] + pho[0] * lit)
        late = CP[0, :, here] * lit
        for i in range(8):
            done = E[i, :, here] + (pho[i] * both + KP[i] * late)
            tout[i, 0, :, here] = done[:4, :]
            tout[i, 0, :, there] = done[4:, :]
        gain = CP[1, :, here]
        for k in range(3):
            H[b, pl.ds(8 * k, 8), :] = (HN[k, :, here] + (KP[8 + k] * both + KP[11 + k] * late)) * gain
        return carry

    lax.fori_loop(0, 16, finish, 0, unroll=4)

    zr_sum = jnp.zeros((24, 128), F32)
    zi_sum = jnp.zeros((24, 128), F32)
    for part in range(2):
        rows = []
        for i in range(4):
            j = 4 * part + i
            rows.append(jnp.concatenate([H[2 * j], H[2 * j + 1]], axis=1))
        spectrum = dot3(jnp.concatenate(rows, axis=0), bh, bl, NT)
        for i in range(4):
            j = 4 * part + i
            ca, sa = [jnp.concatenate([AP[p, j]] * 3, axis=0) for p in range(2)]
            yc = spectrum[24 * i : 24 * i + 24, :128]
            ys = spectrum[24 * i : 24 * i + 24, 128:]
            zr_sum += ca * yc + sa * ys
            zi_sum += ca * ys - sa * yc
    scale = 1.0 / math.sqrt(NLON)
    HF[pl.ds(0, 24), :] = zr_sum * scale
    HF[pl.ds(24, 24), :] = zi_sum * scale
    HF[pl.ds(48, 16), :] = jnp.zeros((16, 128), F32)
    mine = jnp.concatenate(
        [HF[pl.ds(r, 8, stride=8), :] + HF[pl.ds(r + 4, 8, stride=8), :] for r in range(4)], axis=0
    )
    S2[:, pl.ds(0, 32)] = mine.T

    send(S2, 1, G2, gs2, gr2)
    every(S2, G2, gs2, gr2).wait_recv()

    bands = G2[...]
    for r in range(4):
        WT[pl.ds(r, NPOS, stride=4), :] = pltpu.roll(bands, 128 - 8 * r, 1) if r else bands
    weighted = (WT[...].T[:8, :] * quad[...].reshape(1, NLAT)).astype(BF16)
    found = lax.dot_general(weighted, LV[...], NT, preferred_element_type=F32)
    found = jnp.where(degree < NDEG - own_wave, found, 0.0)
    for p in range(2):
        for k in range(3):
            sout[p, k, 0] = found[3 * p + k : 3 * p + k + 1, :]

    every(T, G1, gs, gr).wait_send()
    every(S2, G2, gs2, gr2).wait_send()
    for k in range(NL):
        if k:
            l_copy(k).wait_send()
            p_copy(k).wait_send()
        for side in range(2):
            e_copy(side, k).wait_send()
    for side in range(2):
        h_copy(side).wait_send()


def hand_over(tracers_ref, heating_ref, tracers_out, heating_out, sems):
    copies = [
        pltpu.make_async_copy(tracers_ref, tracers_out, sems.at[0]),
        pltpu.make_async_copy(heating_ref, heating_out, sems.at[1]),
    ]
    for copy in copies:
        copy.start()
    for copy in copies:
        copy.wait()


def body(spectra, legendre, wavenumbers, quad_weights, tracers, kinetics, photolysis, heat_weights):
    vmem = pl.BlockSpec(memory_space=pltpu.VMEM)
    hbm = pl.BlockSpec(memory_space=pl.ANY)
    V, DMA = pltpu.VMEM, pltpu.SemaphoreType.DMA
    tracers_out, heating = pl.pallas_call(
        kernel,
        out_shape=(
            V((8, 1, 4, NLON), F32),
            V((2, 3, 1, 1, NDEG), F32),
        ),
        in_specs=[hbm] * 8,
        out_specs=(vmem, vmem),
        scratch_shapes=[
            V((2, 1, 1, 4, NDEG), BF16), pltpu.SMEM((NPOS,), jnp.int32), V((NLAT,), F32),
            pltpu.SMEM((8, 8), F32), pltpu.SMEM((8,), F32), pltpu.SMEM((3, 8), F32),
            V((8, 8, NLON), F32), V((8, 8, NLON), F32), V((8, 8, NLON // 2), F32), V((8, 8, NLON), F32),
            V((8, 8, NLON // 2), F32), V((8, NLON), F32), V((3, 8, NLON // 2), F32), V((14, 8, 128), F32),
            V((2, 8, NLON // 2), F32), V((2, 8, 8, 128), F32),
            V((NDEG, NLAT), BF16), V((8, NDEG), F32),
            V((NLAT, 128), F32), V((NPOS, 128), F32),
            V((128, 128), F32),
            V((NL, 4, CHUNK), F32), V((NL, 4, CHUNK), F32), V((8, NLON), F32),
            V((6, 8, NLON), F32),
            V((2, 16, 128), F32), V((256, 256), BF16), V((256, 256), BF16),
            V((16, 24, 128), F32), V((64, 128), F32),
            V((128, 128), F32), V((NPOS, 128), F32),
            V((NLAT, 128), F32), V((128, 128), jnp.int32),
            DMA((12,)), DMA((1,)), DMA((1,)), DMA((NL,)), DMA((NL,)),
            DMA((NL,)), DMA((NL,)), DMA((2, NL)), DMA((2, NL)), DMA((2,)), DMA((2,)),
            DMA((1,)), DMA((1,)),
        ],
        compiler_params=pltpu.CompilerParams(collective_id=0, has_side_effects=True),
    )(
        spectra.transpose(0, 2, 3, 1, 4), legendre, wavenumbers, quad_weights, tracers, kinetics,
        photolysis, heat_weights,
    )
    return pl.pallas_call(
        hand_over,
        out_shape=(
            jax.ShapeDtypeStruct((8, 1, 4, NLON), F32),
            jax.ShapeDtypeStruct((2, 3, 1, 1, NDEG), F32),
        ),
        in_specs=[vmem, vmem],
        out_specs=(hbm, hbm),
        scratch_shapes=[DMA((2,))],
    )(
        pltpu.with_memory_space_constraint(tracers_out, pltpu.VMEM),
        pltpu.with_memory_space_constraint(heating, pltpu.VMEM),
    )


def solution(mesh):
    return jax.shard_map(
        body,
        mesh=mesh,
        in_specs=(
            P(None, None, "lev", ("wave", "grp"), None),
            P(("wave", "grp"), None, None),
            P(),
            P(),
            P(None, "lev", ("wave", "grp"), None),
            P(),
            P(),
            P(),
        ),
        out_specs=(
            P(None, "lev", ("wave", "grp"), None),
            P(None, None, "lev", ("wave", "grp"), None),
        ),
        check_vma=False,
    )
```

```python
import math

import jax
import jax.numpy as jnp
from jax import lax
from jax.experimental import pallas as pl
from jax.experimental.pallas import tpu as pltpu
from jax.sharding import PartitionSpec as P

NW, NL, NG = 12, 8, 8
NPOS = NW * NG
NDEG = 1024
NLON = 4096
NLAT = 384
CHUNK = NLON // NL
F32 = jnp.float32
BF16 = jnp.bfloat16
MESH = pl.DeviceIdType.MESH
NT = (((1,), (1,)), ((), ()))
FAR_L = (4, 3, 5, 2, 6, 1, 7)


def wrapped(i, n):
    return jnp.where(i >= n, i - n, i)


def outward(i, n):
    return n // 2 + ((i + 1) >> 1) * (1 - 2 * (i & 1))


def each_peer(w, g, act):
    def row(i, carry):
        for j in range(NG):
            act(wrapped(w + outward(i, NW), NW), wrapped(g + outward(j, NG), NG))
        return carry

    lax.fori_loop(0, NW - 1, row, 0)
    for j in range(NG - 1):
        act(w, wrapped(g + outward(j, NG), NG))


def cos_sin(m):
    shifted = m + NLON // 8
    quarter = (shifted >> 10) & 3
    angle = ((shifted & (NLON // 4 - 1)) - NLON // 8).astype(F32) * (2.0 * math.pi / NLON)
    z = angle * angle
    s = angle * (1.0 + z * (-1.0 / 6 + z * (1.0 / 120 + z * (-1.0 / 5040 + z * (1.0 / 362880)))))
    c = 1.0 + z * (-0.5 + z * (1.0 / 24 + z * (-1.0 / 720 + z * (1.0 / 40320))))
    odd = (quarter & 1) == 1
    cos = jnp.where(odd, s, c)
    sin = jnp.where(odd, c, s)
    cos = jnp.where(((quarter + 1) & 2) == 2, -cos, cos)
    sin = jnp.where((quarter & 2) == 2, -sin, sin)
    return cos, sin


def split(x):
    hi = x.astype(BF16)
    return hi, (x - hi.astype(F32)).astype(BF16)


def dot3(x, bh, bl, dims):
    hi, lo = split(x)
    out = lax.dot_general(hi, bh, dims, preferred_element_type=F32)
    out += lax.dot_general(lo, bh, dims, preferred_element_type=F32)
    return out + lax.dot_general(hi, bl, dims, preferred_element_type=F32)


def kernel(
    spec_in, leg, wn_in, quad_in, trc, kin_in, pho_in, hw_in,
    tout, sout,
    spec, wn, quad, kin, pho, hw, C, D, O, M, E, Q, HN, KP, CP, AP, LV, X, T, G1, V, LR, PC, PH, COEF, AT, BH, BL, H, HF, S2, G2, WT, WC,
    local, gs, gr, ls, lr, ps, pr, es, er, hs, hr, gs2, gr2,
):
    w = lax.axis_index("wave")
    l = lax.axis_index("lev")
    g = lax.axis_index("grp")
    pos = w * NG + g
    up = lax.rem(pos + 1, NPOS)
    down = lax.rem(pos + NPOS - 1, NPOS)
    up_w, up_g = up // NG, lax.rem(up, NG)
    down_w, down_g = down // NG, lax.rem(down, NG)

    for i in range(4):
        rows = pl.ds(256 * i, 256)
        pltpu.make_async_copy(leg.at[0, rows, :], LV.at[rows, :], local.at[i]).start()
    own_rows = pltpu.make_async_copy(trc.at[:, 0], C.at[:, pl.ds(2, 4), :], local.at[4])
    own_rows.start()
    small = [
        pltpu.make_async_copy(src, dst, local.at[6 + i])
        for i, (src, dst) in enumerate(
            ((spec_in, spec), (wn_in, wn), (quad_in, quad), (kin_in, kin), (pho_in, pho), (hw_in, hw))
        )
    ]
    for copy in small:
        copy.start()

    barrier = pltpu.get_barrier_semaphore()

    def hello(dw, dl, dg):
        pl.semaphore_signal(barrier, inc=1, device_id=(dw, dl, dg), device_id_type=MESH)

    each_peer(w, g, lambda dw, dg: hello(dw, l, dg))
    for k in FAR_L:
        ll = wrapped(l + k, NL)
        hello(up_w, ll, up_g)
        hello(down_w, ll, down_g)
        hello(w, ll, g)
    count = NPOS - 1 + 3 * (NL - 1)

    for row in (0, 7):
        PH[pl.ds(row, 1), :] = jnp.zeros((1, NLON), F32)

    small[0].wait()
    small[1].wait()
    own_wave = wn[pos]
    for p in range(2):
        for f in range(4):
            X[pl.ds(4 * p + f, 1), :] = spec[p, 0, 0, pl.ds(f, 1), :].astype(F32)
    degree = lax.broadcasted_iota(jnp.int32, (8, NDEG), 1)
    coeffs = jnp.where(degree < NDEG - own_wave, X[...], 0.0).astype(BF16)
    fourier = jnp.zeros((8, NLAT), F32)
    for i in range(4):
        rows = pl.ds(256 * i, 256)
        pltpu.make_async_copy(leg.at[0, rows, :], LV.at[rows, :], local.at[i]).wait()
        fourier += jnp.dot(
            coeffs[:, 256 * i : 256 * i + 256], LV[rows, :], preferred_element_type=F32
        )
    groups = []
    for r in range(8):
        shift = (NLAT + 2 - r) % NLAT
        groups.append(pltpu.roll(fourier, shift, 1) if shift else fourier)
    T[:, pl.ds(0, 64)] = jnp.concatenate(groups, axis=0).T
    own_rows.wait()

    pl.semaphore_wait(barrier, count)

    def send(src, stride, dst, ssem, rsem):
        def act(there_w, there_g):
            pltpu.make_async_remote_copy(
                src.at[pl.ds((there_w * NG + there_g) * stride, 1)], dst.at[pl.ds(pos, 1)],
                ssem.at[0], rsem.at[0],
                device_id=(there_w, l, there_g), device_id_type=MESH,
            ).start()

        each_peer(w, g, act)
        dst[pl.ds(pos, 1), :] = src[pl.ds(pos * stride, 1), :]

    def every(src, dst, ssem, rsem):
        rows = pl.ds(0, NPOS - 1)
        return pltpu.make_async_remote_copy(
            src.at[rows], dst.at[rows], ssem.at[0], rsem.at[0],
            device_id=(up_w, l, up_g), device_id_type=MESH,
        )

    def l_copy(k, arrival=False):
        there = lax.rem(l + k, NL)
        return pltpu.make_async_remote_copy(
            C.at[0, pl.ds(2, 4), pl.ds(pl.multiple_of(CHUNK * there, CHUNK), CHUNK)],
            LR.at[there if arrival else l], ls.at[k], lr.at[there if arrival else l],
            device_id=(w, there, g), device_id_type=MESH,
        )

    def p_copy(k, arrival=False):
        there = lax.rem(l + k, NL)
        part = there if arrival else l
        return pltpu.make_async_remote_copy(
            PC.at[there],
            PH.at[pl.ds(2, 4), pl.ds(pl.multiple_of(CHUNK * part, CHUNK), CHUNK)],
            ps.at[k], pr.at[part],
            device_id=(w, there, g), device_id_type=MESH,
        )

    def e_copy(side, k, arrival=False):
        there = lax.rem(l + k, NL)
        part = there if arrival else l
        return pltpu.make_async_remote_copy(
            PC.at[there, pl.ds(3 if side else 0, 1)],
            PH.at[pl.ds(1 if side else 6, 1), pl.ds(pl.multiple_of(CHUNK * part, CHUNK), CHUNK)],
            es.at[side, k], er.at[side, part],
            device_id=(up_w, there, up_g) if side else (down_w, there, down_g),
            device_id_type=MESH,
        )

    def h_copy(side):
        return pltpu.make_async_remote_copy(
            C.at[:, pl.ds(4 if side else 2, 2), :],
            C.at[:, pl.ds(0 if side else 6, 2), :],
            hs.at[side], hr.at[side],
            device_id=(up_w, l, up_g) if side else (down_w, l, down_g),
            device_id_type=MESH,
        )

    send(T, 4, G1, gs, gr)
    for k in FAR_L:
        l_copy(k).start()
    for side in range(2):
        h_copy(side).start()
    LR[l] = C[0, pl.ds(2, 4), pl.ds(pl.multiple_of(CHUNK * l, CHUNK), CHUNK)]

    upper = lax.broadcasted_iota(jnp.int32, (8, 256), 0) < 4

    def packed(first, second):
        return jnp.where(
            upper[:, : first.shape[1]], pltpu.roll(first, 6, 0), pltpu.roll(second, 2, 0)
        )

    for k in range(1, NL):
        l_copy(k, True).wait_recv()
    total = jnp.zeros((4, CHUNK), F32)
    for level in range(NL):
        PC[level] = 0.2 * jnp.exp(total * (-2.0 / NL))
        if level < NL - 1:
            total += LR[level]
    for k in FAR_L:
        for side in range(2):
            e_copy(side, k).start()
        p_copy(k).start()
    for side in range(2):
        e_copy(side, 0).start()
    PH[pl.ds(2, 4), pl.ds(pl.multiple_of(CHUNK * l, CHUNK), CHUNK)] = PC[l]

    for s in range(NPOS):
        WC[pl.ds(s, 1), :] = jnp.full((1, 128), wn[s], jnp.int32)
    WC[pl.ds(NPOS, 128 - NPOS), :] = jnp.zeros((128 - NPOS, 128), jnp.int32)
    waves = WC[...]
    across = waves.astype(F32).T[:16, :].astype(jnp.int32)
    coarse = lax.broadcasted_iota(jnp.int32, (16, 128), 0) * 256
    AT[0], AT[1] = cos_sin((across * coarse) & (NLON - 1))
    for p in range(2):
        for j in range(8):
            low = jnp.broadcast_to(AT[p, pl.ds(j, 1), :], (8, 128))
            high = jnp.broadcast_to(AT[p, pl.ds(j + 8, 1), :], (8, 128))
            AP[p, j] = jnp.where(upper[:, :128], low, high)
    used = lax.broadcasted_iota(jnp.int32, (128, 128), 0) < NPOS
    for half in range(2):
        fine = lax.broadcasted_iota(jnp.int32, (128, 128), 1) + 128 * half
        cos, sin = cos_sin((waves * fine) & (NLON - 1))
        for p, table in enumerate((cos, -sin)):
            hi, lo = split(jnp.where(used, table, 0.0))
            BH[pl.ds(128 * p, 128), pl.ds(128 * half, 128)] = hi
            BL[pl.ds(128 * p, 128), pl.ds(128 * half, 128)] = lo

    for copy in small[2:]:
        copy.wait()
    for i in range(8):
        total = jnp.full((8, 128), kin[i, 0] * pho[0], F32)
        for t in range(1, 8):
            total += jnp.full((8, 128), kin[i, t] * pho[t], F32)
        KP[i] = total
    for k in range(3):
        first = jnp.full((8, 128), hw[k, 0] * pho[0], F32)
        second = hw[k, 0] * KP[0]
        for t in range(1, 8):
            first += jnp.full((8, 128), hw[k, t] * pho[t], F32)
            second += hw[k, t] * KP[t]
        KP[8 + k] = first
        KP[11 + k] = second

    for side in range(2):
        h_copy(side).wait_recv()

    @pl.when(pos == 0)
    def _():
        C[:, pl.ds(0, 2), :] = jnp.zeros((8, 2, NLON), F32)

    @pl.when(pos == NPOS - 1)
    def _():
        C[:, pl.ds(6, 2), :] = jnp.zeros((8, 2, NLON), F32)

    every(T, G1, gs, gr).wait_recv()

    arrived = jnp.concatenate([G1[...], jnp.zeros((128 - NPOS, 128), F32)], axis=0)
    V[...] = arrived.T
    parts = []
    for p in range(2):
        fields = [V[pl.ds(4 * p + f, 8, stride=8), :] for f in range(4)]
        parts.append(jnp.concatenate(fields, axis=0) * (1.0 / math.sqrt(NPOS)))
    real, imag = parts
    latitude = lax.broadcasted_iota(jnp.int32, (8, 256), 0) + (4 * pos - 2)
    inside = jnp.where((latitude >= 0) & (latitude < NLAT), 1.0, 0.0)
    bh, bl = BH[...], BL[...]
    for part in range(4):
        blocks = (2 * part, 2 * part + 1, 2 * part + 8, 2 * part + 9)
        turned = []
        for h in blocks:
            ca, sa = AT[0, pl.ds(h, 1), :], AT[1, pl.ds(h, 1), :]
            turned.append(
                jnp.concatenate([real * ca - imag * sa, real * sa + imag * ca], axis=1)
            )
        grid = dot3(jnp.concatenate(turned, axis=0), bh, bl, (((1,), (0,)), ((), ())))
        rates, gains = [], []
        for i, h in enumerate(blocks):
            cols = pl.ds(256 * h, 256)
            field = [grid[32 * i + 8 * f : 32 * i + 8 * f + 8, :] for f in range(4)]
            cx = 0.45 * jnp.tanh(field[0]) * inside
            cy = 0.45 * jnp.tanh(field[1]) * inside
            COEF[0, :, cols] = inside - jnp.abs(cx) - jnp.abs(cy)
            COEF[1, :, cols] = jnp.maximum(cx, 0.0)
            COEF[2, :, cols] = jnp.maximum(-cx, 0.0)
            COEF[3, :, cols] = jnp.maximum(cy, 0.0)
            COEF[4, :, cols] = jnp.maximum(-cy, 0.0)
            rates.append(0.2 * jnp.exp(0.3 * field[2]))
            COEF[5, :, cols] = rates[i]
            gains.append(field[3])
        for i in range(2):
            cols = pl.ds(256 * blocks[i], 256)
            CP[0, :, cols] = packed(rates[i], rates[i + 2])
            CP[1, :, cols] = 1.0 + 0.5 * jnp.tanh(packed(gains[i], gains[i + 2]))

    lane = lax.broadcasted_iota(jnp.int32, (8, 128), 1)

    def transported(b, pick):
        west = pl.ds(pl.multiple_of(((b + 31) & 31) * 128, 128), 128)
        east = pl.ds(pl.multiple_of(((b + 1) & 31) * 128, 128), 128)
        here = pl.ds(pl.multiple_of(b * 128, 128), 128)
        cc, xp, xm, yp, ym = [COEF[i, :, here] for i in range(5)]

        def of(t):
            c = pick(t, here)
            western = pltpu.roll(jnp.where(lane == 127, pick(t, west), c), 1, 1)
            eastern = pltpu.roll(jnp.where(lane == 0, pick(t, east), c), 127, 1)
            northern = pltpu.roll(c, 1, 0)
            southern = pltpu.roll(c, 7, 0)
            return cc * c + xp * western + xm * eastern + yp * northern + ym * southern

        return of

    def transport(b, carry):
        of = transported(b, lambda t, cols: C[t, :, cols])
        for t in range(8):
            M[t, :, pl.ds(pl.multiple_of(b * 128, 128), 128)] = of(t)
        return carry

    def transport_packed(b, carry):
        first = transported(b, lambda t, cols: D[t, :, cols])
        second = transported(b + 16, lambda t, cols: D[t, :, cols])
        for t in range(8):
            O[t, :, pl.ds(pl.multiple_of(b * 128, 128), 128)] = packed(first(t), second(t))
        return carry

    def mix(src, rates, dst, heats):
        def block(b, carry):
            cols = pl.ds(pl.multiple_of(b * 512, 512), 512)
            rate = rates[:, cols]
            moved = [src[t, :, cols] for t in range(8)]
            heat = [None] * 3
            for i in range(8):
                mixed = kin[i, 0] * moved[0]
                for t in range(1, 8):
                    mixed += kin[i, t] * moved[t]
                done = moved[i] + rate * mixed
                dst[i, :, cols] = done
                if heats:
                    heat = [
                        hw[k, i] * done if old is None else old + hw[k, i] * done
                        for k, old in enumerate(heat)
                    ]
            if heats:
                for k in range(3):
                    HN[k, :, cols] = heat[k]
            return carry

        lax.fori_loop(0, dst.shape[2] // 512, block, 0)

    lax.fori_loop(0, 32, transport, 0, unroll=16)
    mix(M, COEF.at[5], D, False)
    lax.fori_loop(0, 16, transport_packed, 0, unroll=8)
    mix(O, CP.at[0], E, True)
    for k in range(NL):
        if k:
            p_copy(k, True).wait_recv()
        for side in range(2):
            e_copy(side, k, True).wait_recv()
    Q[...] = PH[...] * M[0]

    def finish(b, carry):
        here = pl.ds(pl.multiple_of(b * 128, 128), 128)
        there = pl.ds(pl.multiple_of(b * 128 + 2048, 128), 128)
        lit = packed(
            transported(b, lambda t, cols: Q[:, cols])(0),
            transported(b + 16, lambda t, cols: Q[:, cols])(0),
        )
        light = packed(PH[:, here], PH[:, there])
        both = lit + light * (O[0, :, here] + pho[0] * lit)
        late = CP[0, :, here] * lit
        for i in range(8):
            done = E[i, :, here] + (pho[i] * both + KP[i] * late)
            tout[i, 0, :, here] = done[:4, :]
            tout[i, 0, :, there] = done[4:, :]
        gain = CP[1, :, here]
        for k in range(3):
            H[b, pl.ds(8 * k, 8), :] = (HN[k, :, here] + (KP[8 + k] * both + KP[11 + k] * late)) * gain
        return carry

    lax.fori_loop(0, 16, finish, 0, unroll=4)

    zr_sum = jnp.zeros((24, 128), F32)
    zi_sum = jnp.zeros((24, 128), F32)
    for part in range(2):
        rows = []
        for i in range(4):
            j = 4 * part + i
            rows.append(jnp.concatenate([H[2 * j], H[2 * j + 1]], axis=1))
        spectrum = dot3(jnp.concatenate(rows, axis=0), bh, bl, NT)
        for i in range(4):
            j = 4 * part + i
            ca, sa = [jnp.concatenate([AP[p, j]] * 3, axis=0) for p in range(2)]
            yc = spectrum[24 * i : 24 * i + 24, :128]
            ys = spectrum[24 * i : 24 * i + 24, 128:]
            zr_sum += ca * yc + sa * ys
            zi_sum += ca * ys - sa * yc
    scale = 1.0 / math.sqrt(NLON)
    HF[pl.ds(0, 24), :] = zr_sum * scale
    HF[pl.ds(24, 24), :] = zi_sum * scale
    HF[pl.ds(48, 16), :] = jnp.zeros((16, 128), F32)
    mine = jnp.concatenate(
        [HF[pl.ds(r, 8, stride=8), :] + HF[pl.ds(r + 4, 8, stride=8), :] for r in range(4)], axis=0
    )
    S2[:, pl.ds(0, 32)] = mine.T

    send(S2, 1, G2, gs2, gr2)
    every(S2, G2, gs2, gr2).wait_recv()

    bands = G2[...]
    for r in range(4):
        WT[pl.ds(r, NPOS, stride=4), :] = pltpu.roll(bands, 128 - 8 * r, 1) if r else bands
    weighted = (WT[...].T[:8, :] * quad[...].reshape(1, NLAT)).astype(BF16)
    found = lax.dot_general(weighted, LV[...], NT, preferred_element_type=F32)
    found = jnp.where(degree < NDEG - own_wave, found, 0.0)
    for p in range(2):
        for k in range(3):
            sout[p, k, 0] = found[3 * p + k : 3 * p + k + 1, :]

    every(T, G1, gs, gr).wait_send()
    every(S2, G2, gs2, gr2).wait_send()
    for k in range(NL):
        if k:
            l_copy(k).wait_send()
            p_copy(k).wait_send()
        for side in range(2):
            e_copy(side, k).wait_send()
    for side in range(2):
        h_copy(side).wait_send()


def hand_over(tracers_ref, heating_ref, tracers_out, heating_out, sems):
    copies = [
        pltpu.make_async_copy(tracers_ref, tracers_out, sems.at[0]),
        pltpu.make_async_copy(heating_ref, heating_out, sems.at[1]),
    ]
    for copy in copies:
        copy.start()
    for copy in copies:
        copy.wait()


def body(spectra, legendre, wavenumbers, quad_weights, tracers, kinetics, photolysis, heat_weights):
    vmem = pl.BlockSpec(memory_space=pltpu.VMEM)
    hbm = pl.BlockSpec(memory_space=pl.ANY)
    V, DMA = pltpu.VMEM, pltpu.SemaphoreType.DMA
    tracers_out, heating = pl.pallas_call(
        kernel,
        out_shape=(
            V((8, 1, 4, NLON), F32),
            V((2, 3, 1, 1, NDEG), F32),
        ),
        in_specs=[hbm] * 8,
        out_specs=(vmem, vmem),
        scratch_shapes=[
            V((2, 1, 1, 4, NDEG), BF16), pltpu.SMEM((NPOS,), jnp.int32), V((NLAT,), F32),
            pltpu.SMEM((8, 8), F32), pltpu.SMEM((8,), F32), pltpu.SMEM((3, 8), F32),
            V((8, 8, NLON), F32), V((8, 8, NLON), F32), V((8, 8, NLON // 2), F32), V((8, 8, NLON), F32),
            V((8, 8, NLON // 2), F32), V((8, NLON), F32), V((3, 8, NLON // 2), F32), V((14, 8, 128), F32),
            V((2, 8, NLON // 2), F32), V((2, 8, 8, 128), F32),
            V((NDEG, NLAT), BF16), V((8, NDEG), F32),
            V((NLAT, 128), F32), V((NPOS, 128), F32),
            V((128, 128), F32),
            V((NL, 4, CHUNK), F32), V((NL, 4, CHUNK), F32), V((8, NLON), F32),
            V((6, 8, NLON), F32),
            V((2, 16, 128), F32), V((256, 256), BF16), V((256, 256), BF16),
            V((16, 24, 128), F32), V((64, 128), F32),
            V((128, 128), F32), V((NPOS, 128), F32),
            V((NLAT, 128), F32), V((128, 128), jnp.int32),
            DMA((12,)), DMA((1,)), DMA((1,)), DMA((NL,)), DMA((NL,)),
            DMA((NL,)), DMA((NL,)), DMA((2, NL)), DMA((2, NL)), DMA((2,)), DMA((2,)),
            DMA((1,)), DMA((1,)),
        ],
        compiler_params=pltpu.CompilerParams(collective_id=0, has_side_effects=True),
    )(
        spectra.transpose(0, 2, 3, 1, 4), legendre, wavenumbers, quad_weights, tracers, kinetics,
        photolysis, heat_weights,
    )
    return pl.pallas_call(
        hand_over,
        out_shape=(
            jax.ShapeDtypeStruct((8, 1, 4, NLON), F32),
            jax.ShapeDtypeStruct((2, 3, 1, 1, NDEG), F32),
        ),
        in_specs=[vmem, vmem],
        out_specs=(hbm, hbm),
        scratch_shapes=[DMA((2,))],
    )(
        pltpu.with_memory_space_constraint(tracers_out, pltpu.VMEM),
        pltpu.with_memory_space_constraint(heating, pltpu.VMEM),
    )


def solution(mesh):
    return jax.shard_map(
        body,
        mesh=mesh,
        in_specs=(
            P(None, None, "lev", ("wave", "grp"), None),
            P(("wave", "grp"), None, None),
            P(),
            P(),
            P(None, "lev", ("wave", "grp"), None),
            P(),
            P(),
            P(),
        ),
        out_specs=(
            P(None, "lev", ("wave", "grp"), None),
            P(None, None, "lev", ("wave", "grp"), None),
        ),
        check_vma=False,
    )
```
